8 devices in a mesh: dp: 1 (over z), tp: 2 (over y), sq: 4 (over x, core).
Axes of the slice: x: 2, y: 2, z: 1, core: 2. Of those that a mesh axis runs over, the one named last changes fastest.
Arguments:
- hidden: bfloat16 [256, 2048], P('dp')
- cache_lens: int32 [256], P('dp')
- k_cache: bfloat16 [256, 1024, 128], P('dp', 'sq')
- v_cache: bfloat16 [256, 1024, 128], P('dp', 'sq')
- ln_gain: float32 [2048], replicated
- ln_bias: float32 [2048], replicated
- w_query: bfloat16 [2048, 2048], P(None, 'tp')
- b_query: float32 [2048], P('tp')
- w_kv: bfloat16 [2048, 256], replicated
- b_kv: float32 [256], replicated
- w_out: bfloat16 [2048, 2048], P('tp')
- b_out: float32 [2048], replicated
Outputs:
- output 1: bfloat16 [256, 2048], P('dp')
- output 2: bfloat16 [256, 1024, 128], P('dp', 'sq')
- output 3: bfloat16 [256, 1024, 128], P('dp', 'sq')
All inputs are finite; a program needn't handle non-finite values.
Results may differ from the reference program's by a relative error of at most 0.00351369.
Values sent between devices are 32-bit elements.
A program may use at most 1 GiB of HBM per device.

```python
import math
import jax
import jax.numpy as jnp
from jax import lax

BATCH = 256
CACHE_LEN = 1024
D_MODEL = 2048
HEADS = 16
HEAD_DIM = 128


def layer_norm(x_rows, ln_gain, ln_bias):
    x_wide = x_rows.astype(jnp.float32)
    mean_val = jnp.mean(x_wide, axis=-1, keepdims=True)
    centered = x_wide - mean_val
    variance = jnp.mean(centered * centered, axis=-1, keepdims=True)
    normed = centered * lax.rsqrt(variance + 1e-5)
    return (normed * ln_gain + ln_bias).astype(jnp.bfloat16)


def setup_inputs(seed: int = 0, part: int = 0) -> dict:
    own_keys = jax.random.split(jax.random.fold_in(jax.random.key(seed), part), 5)
    shared_keys = jax.random.split(jax.random.key(seed + 1), 10)
    q_width = HEADS * HEAD_DIM
    score_var = max(1.0, math.log(CACHE_LEN / 32.0))
    key_scale = math.sqrt(score_var / 2.0)
    self_bias = (math.log(0.6 * CACHE_LEN) + 0.5 * score_var) / math.sqrt(HEAD_DIM)
    hidden = jax.random.normal(own_keys[0], (BATCH, D_MODEL), jnp.float32).astype(jnp.bfloat16)
    drawn = CACHE_LEN - 1 - jax.random.randint(own_keys[1], (BATCH,), 0, CACHE_LEN // 2)
    order = jax.random.permutation(own_keys[2], BATCH)
    seq_ids = jnp.arange(BATCH)
    cache_lens = jnp.where(seq_ids == order[0], CACHE_LEN - 1, jnp.where(seq_ids == order[1], 1, drawn)).astype(jnp.int32)
    k_cache = (key_scale * jax.random.normal(own_keys[3], (BATCH, CACHE_LEN, HEAD_DIM), jnp.float32)).astype(jnp.bfloat16)
    v_cache = jax.random.normal(own_keys[4], (BATCH, CACHE_LEN, HEAD_DIM), jnp.float32).astype(jnp.bfloat16)
    ln_gain = 1.0 + 0.3 * jax.random.normal(shared_keys[0], (D_MODEL,), jnp.float32)
    ln_bias = 0.3 * jax.random.normal(shared_keys[1], (D_MODEL,), jnp.float32)
    w_query = (jax.random.normal(shared_keys[2], (D_MODEL, q_width), jnp.float32) * D_MODEL ** -0.5).astype(jnp.bfloat16)
    shared_dir = jax.random.normal(shared_keys[3], (HEAD_DIM,), jnp.float32)
    b_query = jnp.tile(shared_dir, HEADS) + 0.2 * jax.random.normal(shared_keys[4], (q_width,), jnp.float32)
    w_kv = (jax.random.normal(shared_keys[5], (D_MODEL, 2 * HEAD_DIM), jnp.float32) * D_MODEL ** -0.5).astype(jnp.bfloat16)
    key_bias = self_bias * shared_dir + 0.2 * jax.random.normal(shared_keys[6], (HEAD_DIM,), jnp.float32)
    val_bias = 0.5 * jax.random.normal(shared_keys[7], (HEAD_DIM,), jnp.float32)
    b_kv = jnp.concatenate([key_bias, val_bias])
    w_out = (jax.random.normal(shared_keys[8], (q_width, D_MODEL), jnp.float32) * q_width ** -0.5).astype(jnp.bfloat16)
    b_out = 0.3 * jax.random.normal(shared_keys[9], (D_MODEL,), jnp.float32)
    return {"hidden": hidden, "cache_lens": cache_lens, "k_cache": k_cache, "v_cache": v_cache, "ln_gain": ln_gain, "ln_bias": ln_bias, "w_query": w_query, "b_query": b_query, "w_kv": w_kv, "b_kv": b_kv, "w_out": w_out, "b_out": b_out}


def reference(hidden, cache_lens, k_cache, v_cache, ln_gain, ln_bias, w_query, b_query, w_kv, b_kv, w_out, b_out):
    normed = layer_norm(hidden, ln_gain, ln_bias)
    query = (jnp.dot(normed, w_query, preferred_element_type=jnp.float32) + b_query).astype(jnp.bfloat16)
    query = query.reshape(BATCH, HEADS, HEAD_DIM)
    key_val = (jnp.dot(normed, w_kv, preferred_element_type=jnp.float32) + b_kv).astype(jnp.bfloat16)
    positions = jnp.arange(CACHE_LEN, dtype=jnp.int32)
    at_slot = (positions[None, :] == cache_lens[:, None])[:, :, None]
    key_new = jnp.where(at_slot, key_val[:, None, :HEAD_DIM], k_cache)
    val_new = jnp.where(at_slot, key_val[:, None, HEAD_DIM:], v_cache)

    def one_sequence(packed):
        query_row, key_rows, val_rows, length = packed
        scores = jnp.einsum("nd,td->nt", query_row.astype(jnp.float32), key_rows.astype(jnp.float32)) * (HEAD_DIM ** -0.5)
        valid = positions <= length
        scores = jnp.where(valid[None, :], scores, -jnp.inf)
        weights = jax.nn.softmax(scores, axis=-1)
        return jnp.einsum("nt,td->nd", weights, val_rows.astype(jnp.float32)).astype(jnp.bfloat16)

    attended = lax.map(one_sequence, (query, key_new, val_new, cache_lens))
    projected = jnp.dot(attended.reshape(BATCH, HEADS * HEAD_DIM), w_out, preferred_element_type=jnp.float32)
    out_hidden = (hidden.astype(jnp.float32) + projected + b_out).astype(jnp.bfloat16)
    return (out_hidden, key_new, val_new)
```

```python
import functools
import jax
import jax.numpy as jnp
from jax import lax
from jax.experimental import pallas as pl
from jax.experimental.pallas import tpu as pltpu
from jax.sharding import PartitionSpec as P

MESH = pl.DeviceIdType.MESH
F32, BF16 = jnp.float32, jnp.bfloat16
CHUNK = 8
SLOTS = 24
LEAD = 16
HEAD = 128
LANES = 128


def attend_kernel(seqs, lens, x_hbm, kc, vc, gain, bias, wq_hbm, bq, wkv_hbm, bkv, kn, vn, num, stat,
                  x_s, h_s, wq_s, wkv_s, q_s, kv_s, kbuf, vbuf, sem_in, rk, rv, wk, wv):
    pos = kc.shape[1]
    heads = q_s.shape[1]
    chunks = seqs // CHUNK
    me = lax.axis_index("sq")
    base = me * pos

    def read(i):
        s = lax.rem(i, SLOTS)
        rows = pl.ds(i * CHUNK, CHUNK)
        return (pltpu.make_async_copy(kc.at[rows], kbuf.at[s], rk.at[s]),
                pltpu.make_async_copy(vc.at[rows], vbuf.at[s], rv.at[s]))

    def write(i):
        s = lax.rem(i, SLOTS)
        rows = pl.ds(i * CHUNK, CHUNK)
        return (pltpu.make_async_copy(kbuf.at[s], kn.at[rows], wk.at[s]),
                pltpu.make_async_copy(vbuf.at[s], vn.at[rows], wv.at[s]))

    parts = wq_hbm.shape[1] // 256
    in_x = pltpu.make_async_copy(x_hbm, x_s, sem_in.at[0])
    in_kv = pltpu.make_async_copy(wkv_hbm, wkv_s, sem_in.at[1])
    in_q = [pltpu.make_async_copy(wq_hbm.at[:, pl.ds(g * 256, 256)], wq_s.at[:, pl.ds(g * 256, 256)], sem_in.at[2 + g])
            for g in range(parts)]
    in_x.start()
    in_kv.start()
    for c in in_q:
        c.start()

    @pl.loop(0, LEAD)
    def _(i):
        for c in read(i):
            c.start()

    in_x.wait()
    rows_n = 32

    @pl.loop(0, x_s.shape[0] // rows_n)
    def _(r):
        rows = pl.ds(r * rows_n, rows_n)
        wide = x_s[rows, :].astype(F32)
        mean = jnp.mean(wide, axis=-1, keepdims=True)
        cent = wide - mean
        var = jnp.mean(cent * cent, axis=-1, keepdims=True)
        h_s[rows, :] = (cent * lax.rsqrt(var + 1e-5) * gain[...] + bias[...]).astype(BF16)

    in_kv.wait()
    kv_s[...] = (jnp.dot(h_s[...], wkv_s[...], preferred_element_type=F32) + bkv[...]).astype(BF16).astype(F32)
    for g in range(parts):
        in_q[g].wait()
        cols = slice(g * 256, (g + 1) * 256)
        q = (jnp.dot(h_s[...], wq_s[:, cols], preferred_element_type=F32) + bq[:, cols]).astype(BF16).astype(F32)
        q_s[:, 2 * g, :] = q[:, :HEAD]
        q_s[:, 2 * g + 1, :] = q[:, HEAD:]

    spot = lax.broadcasted_iota(jnp.int32, (heads, pos), 1) + base
    lane = lax.broadcasted_iota(jnp.int32, (heads, LANES), 1)
    row16 = lax.broadcasted_iota(jnp.int32, (16, HEAD), 0)
    stat[...] = jnp.zeros_like(stat)
    own = seqs // 4

    @pl.loop(0, chunks)
    def _(i):
        s = lax.rem(i, SLOTS)
        for c in read(i):
            c.wait()
        first = i * CHUNK
        for j in range(CHUNK):
            b = first + j
            slot = lens[b] - base
            inside = jnp.logical_and(slot >= 0, slot < pos)
            at = pl.multiple_of(jnp.where(inside, slot // 16, 0) * 16, 16)
            mark = row16 == jnp.where(inside, slot - at, -1)
            win = pl.ds(at, 16)
            new = kv_s[pl.ds(b, 1), :].astype(BF16)
            kbuf[s, j, win, :] = jnp.where(mark, new[:, :HEAD], kbuf[s, j, win, :])
            vbuf[s, j, win, :] = jnp.where(mark, new[:, HEAD:], vbuf[s, j, win, :])
        group = first // own
        off = first - group * own
        tops, sums = stat[group, 0], stat[group, 1]
        for j in range(CHUNK):
            b = first + j
            q = q_s[b].astype(BF16)
            sc = lax.dot_general(q, kbuf[s, j], (((1,), (1,)), ((), ())), preferred_element_type=F32) * (HEAD ** -0.5)
            valid = spot <= lens[b]
            sc = jnp.where(valid, sc, -1e30)
            top = jnp.max(sc, axis=1, keepdims=True)
            w = jnp.where(valid, jnp.exp(sc - top), 0.0)
            tot = jnp.sum(w, axis=1, keepdims=True)
            num[b] = jnp.dot(w.astype(BF16), vbuf[s, j], preferred_element_type=F32)
            tops = jnp.where(lane == off + j, top, tops)
            sums = jnp.where(lane == off + j, tot, sums)
        stat[group, 0] = tops
        stat[group, 1] = sums
        for c in write(i):
            c.start()
        ahead = i + LEAD

        @pl.when(ahead < chunks)
        def _():
            @pl.when(ahead >= SLOTS)
            def _():
                for c in write(ahead - SLOTS):
                    c.wait()
            for c in read(ahead):
                c.start()

    @pl.loop(max(0, chunks - SLOTS), chunks)
    def _(i):
        for c in write(i):
            c.wait()


def attend(lens, x, kc, vc, gain, bias, wq, bq, wkv, bkv):
    seqs, pos, _ = kc.shape
    heads = wq.shape[1] // HEAD
    width = x.shape[1]
    hbm = pl.BlockSpec(memory_space=pl.ANY)
    vmem = pl.BlockSpec(memory_space=pltpu.VMEM)
    smem = pl.BlockSpec(memory_space=pltpu.SMEM)
    return pl.pallas_call(
        functools.partial(attend_kernel, seqs),
        out_shape=(jax.ShapeDtypeStruct(kc.shape, BF16), jax.ShapeDtypeStruct(vc.shape, BF16),
                   jax.ShapeDtypeStruct((seqs, heads, HEAD), F32), jax.ShapeDtypeStruct((4, 2, heads, LANES), F32)),
        in_specs=[smem, hbm, hbm, hbm, vmem, vmem, hbm, vmem, hbm, vmem],
        out_specs=(hbm, hbm, vmem, vmem),
        scratch_shapes=[
            pltpu.VMEM((seqs, width), BF16), pltpu.VMEM((seqs, width), BF16), pltpu.VMEM(wq.shape, BF16),
            pltpu.VMEM(wkv.shape, BF16), pltpu.VMEM((seqs, heads, HEAD), F32), pltpu.VMEM((seqs, 2 * HEAD), F32),
            pltpu.VMEM((SLOTS, CHUNK, pos, HEAD), BF16), pltpu.VMEM((SLOTS, CHUNK, pos, HEAD), BF16),
            pltpu.SemaphoreType.DMA((8,)), pltpu.SemaphoreType.DMA((SLOTS,)), pltpu.SemaphoreType.DMA((SLOTS,)),
            pltpu.SemaphoreType.DMA((SLOTS,)), pltpu.SemaphoreType.DMA((SLOTS,)),
        ],
        compiler_params=pltpu.CompilerParams(vmem_limit_bytes=60 * 1024 * 1024),
        name="attend",
    )(lens, x, kc, vc, gain[None], bias[None], wq, bq[None], wkv, bkv[None])


def solution(mesh):
    def local_step(hidden, cache_lens, k_cache, v_cache, ln_gain, ln_bias, w_query, b_query, w_kv, b_kv, w_out, b_out):
        key_new, val_new, num, stat = attend(cache_lens, hidden, k_cache, v_cache, ln_gain, ln_bias, w_query, b_query, w_kv, b_kv)
        seqs, heads, _ = num.shape
        own = seqs // 4
        tops = stat[:, 0, :, :own].transpose(0, 2, 1).reshape(seqs, heads, 1)
        sums = stat[:, 1, :, :own].transpose(0, 2, 1).reshape(seqs, heads, 1)
        best = lax.pmax(tops, "sq")
        scale = jnp.exp(tops - best)
        den = lax.psum(sums * scale, "sq")
        full = lax.psum(num * scale, "sq")
        attended = (full / den).astype(BF16).reshape(seqs, heads * HEAD)
        projected = lax.psum(jnp.dot(attended, w_out, preferred_element_type=F32), "tp")
        out = (hidden.astype(F32) + projected + b_out).astype(BF16)
        return out, key_new, val_new

    cache_spec = P("dp", "sq", None)
    row_spec = P("dp", None)
    in_specs = (row_spec, P("dp"), cache_spec, cache_spec, P(None), P(None), P(None, "tp"), P("tp"), P(None, None), P(None), P("tp", None), P(None))
    out_specs = (row_spec, cache_spec, cache_spec)
    return jax.shard_map(local_step, mesh=mesh, in_specs=in_specs, out_specs=out_specs, check_vma=False)
```

```python
import functools
import jax
import jax.numpy as jnp
from jax import lax
from jax.experimental import pallas as pl
from jax.experimental.pallas import tpu as pltpu
from jax.sharding import PartitionSpec as P

MESH = pl.DeviceIdType.MESH
F32, BF16 = jnp.float32, jnp.bfloat16
CHUNK = 16
SLOTS = 14
LEAD = 9
UNIT = 8
GROUPS = CHUNK // UNIT
HEAD = 128
LANES = 128


def attend_kernel(seqs, lens_hbm, x_hbm, kc, vc, gain_hbm, bias_hbm, wq_hbm, bq_hbm, wkv_hbm, bkv_hbm, kn, vn, part,
                  lens, gain, bias, bq, bkv, x_s, h_s, wq_s, wkv_s, q_s, kv_s, kbuf, vbuf, sem_in, rk, rv, wk, wv):
    pos = kc.shape[1]
    heads = q_s.shape[1]
    chunks = seqs // CHUNK
    me = lax.axis_index("sq")
    base = me * pos

    def read(i):
        s = lax.rem(i, SLOTS)
        rows = pl.ds(i * CHUNK, CHUNK)
        return (pltpu.make_async_copy(kc.at[rows], kbuf.at[s], rk.at[s]),
                pltpu.make_async_copy(vc.at[rows], vbuf.at[s], rv.at[s]))

    def write(i):
        s = lax.rem(i, SLOTS)
        rows = pl.ds(i * CHUNK, CHUNK)
        return (pltpu.make_async_copy(kbuf.at[s], kn.at[rows], wk.at[s]),
                pltpu.make_async_copy(vbuf.at[s], vn.at[rows], wv.at[s]))

    parts = wq_hbm.shape[1] // 256
    in_x = pltpu.make_async_copy(x_hbm, x_s, sem_in.at[0])
    in_kv = pltpu.make_async_copy(wkv_hbm, wkv_s, sem_in.at[1])
    in_q = [pltpu.make_async_copy(wq_hbm.at[:, pl.ds(g * 256, 256)], wq_s.at[:, pl.ds(g * 256, 256)], sem_in.at[2 + g])
            for g in range(parts)]
    small = [pltpu.make_async_copy(a, b, sem_in.at[8 + n])
             for n, (a, b) in enumerate(((gain_hbm, gain), (bias_hbm, bias), (bkv_hbm, bkv), (bq_hbm, bq), (lens_hbm, lens)))]
    in_x.start()
    for c in small:
        c.start()
    in_kv.start()
    for c in in_q:
        c.start()

    @pl.loop(0, LEAD)
    def _(i):
        for c in read(i):
            c.start()

    in_x.wait()
    for c in small:
        c.wait()
    rows_n = 32

    @pl.loop(0, x_s.shape[0] // rows_n)
    def _(r):
        rows = pl.ds(r * rows_n, rows_n)
        wide = x_s[rows, :].astype(F32)
        mean = jnp.mean(wide, axis=-1, keepdims=True)
        cent = wide - mean
        var = jnp.mean(cent * cent, axis=-1, keepdims=True)
        h_s[rows, :] = (cent * lax.rsqrt(var + 1e-5) * gain[...] + bias[...]).astype(BF16)

    in_kv.wait()
    kv_s[...] = (jnp.dot(h_s[...], wkv_s[...], preferred_element_type=F32) + bkv[...]).astype(BF16).astype(F32)
    for g in range(parts):
        in_q[g].wait()
        cols = slice(g * 256, (g + 1) * 256)
        q = (jnp.dot(h_s[...], wq_s[:, cols], preferred_element_type=F32) + bq[:, cols]).astype(BF16).astype(F32)
        q_s[:, 2 * g, :] = q[:, :HEAD]
        q_s[:, 2 * g + 1, :] = q[:, HEAD:]

    spot = lax.broadcasted_iota(jnp.int32, (heads, pos), 1) + base
    lane = lax.broadcasted_iota(jnp.int32, (heads, LANES), 1)
    row16 = lax.broadcasted_iota(jnp.int32, (16, HEAD), 0)
    def spread(i):
        return pl.multiple_of(i * CHUNK, CHUNK), lax.rem(i, SLOTS)

    def values(i, weights):
        first, s = spread(i)
        for j in range(CHUNK):
            part[i * GROUPS + j // UNIT, j % UNIT] = jnp.dot(weights[j], vbuf[s, j], preferred_element_type=F32)

    def body(i, weights):
        first, s = spread(i)
        for c in read(i):
            c.wait()
        for j in range(CHUNK):
            b = first + j
            slot = lens[b] - base
            inside = jnp.logical_and(slot >= 0, slot < pos)
            at = pl.multiple_of(jnp.where(inside, slot // 16, 0) * 16, 16)
            mark = row16 == jnp.where(inside, slot - at, -1)
            win = pl.ds(at, 16)
            new = kv_s[pl.ds(b, 1), :].astype(BF16)
            kbuf[s, j, win, :] = jnp.where(mark, new[:, :HEAD], kbuf[s, j, win, :])
            vbuf[s, j, win, :] = jnp.where(mark, new[:, HEAD:], vbuf[s, j, win, :])
        scores = [lax.dot_general(q_s[first + j].astype(BF16), kbuf[s, j], (((1,), (1,)), ((), ())), preferred_element_type=F32)
                  for j in range(CHUNK)]
        values(jnp.maximum(i - 1, 0), weights)
        out = []
        for g in range(GROUPS):
            stat = jnp.zeros((heads, LANES), F32)
            for j in range(UNIT):
                valid = spot <= lens[first + g * UNIT + j]
                sc = jnp.where(valid, scores[g * UNIT + j] * (HEAD ** -0.5), -1e30)
                top = jnp.max(sc, axis=1, keepdims=True)
                w = jnp.where(valid, jnp.exp(sc - top), 0.0)
                tot = jnp.sum(w, axis=1, keepdims=True)
                out.append(w.astype(BF16))
                stat = jnp.where(lane == j, top, jnp.where(lane == UNIT + j, tot, stat))
            part[i * GROUPS + g, UNIT] = stat
        for c in write(i):
            c.start()
        ahead = i + LEAD

        @pl.when(ahead < chunks)
        def _():
            @pl.when(ahead >= SLOTS)
            def _():
                for c in write(ahead - SLOTS):
                    c.wait()
            for c in read(ahead):
                c.start()

        return tuple(out)

    last = lax.fori_loop(0, chunks, body, tuple(jnp.zeros((heads, pos), BF16) for _ in range(CHUNK)))
    values(chunks - 1, last)

    @pl.loop(max(0, chunks - SLOTS), chunks)
    def _(i):
        for c in write(i):
            c.wait()


def attend(lens, x, kc, vc, gain, bias, wq, bq, wkv, bkv):
    seqs, pos, _ = kc.shape
    heads = wq.shape[1] // HEAD
    width = x.shape[1]
    hbm = pl.BlockSpec(memory_space=pltpu.HBM)
    vmem = pl.BlockSpec(memory_space=pltpu.VMEM)
    return pl.pallas_call(
        functools.partial(attend_kernel, seqs),
        out_shape=(jax.ShapeDtypeStruct(kc.shape, BF16), jax.ShapeDtypeStruct(vc.shape, BF16),
                   jax.ShapeDtypeStruct((seqs // UNIT, UNIT + 1, heads, HEAD), F32)),
        in_specs=[hbm] * 10,
        out_specs=(hbm, hbm, vmem),
        scratch_shapes=[
            pltpu.SMEM((seqs,), jnp.int32), pltpu.VMEM((1, width), F32), pltpu.VMEM((1, width), F32),
            pltpu.VMEM((1, wq.shape[1]), F32), pltpu.VMEM((1, 2 * HEAD), F32),
            pltpu.VMEM((seqs, width), BF16), pltpu.VMEM((seqs, width), BF16), pltpu.VMEM(wq.shape, BF16),
            pltpu.VMEM(wkv.shape, BF16), pltpu.VMEM((seqs, heads, HEAD), F32), pltpu.VMEM((seqs, 2 * HEAD), F32),
            pltpu.VMEM((SLOTS, CHUNK, pos, HEAD), BF16), pltpu.VMEM((SLOTS, CHUNK, pos, HEAD), BF16),
            pltpu.SemaphoreType.DMA((13,)), pltpu.SemaphoreType.DMA((SLOTS,)), pltpu.SemaphoreType.DMA((SLOTS,)),
            pltpu.SemaphoreType.DMA((SLOTS,)), pltpu.SemaphoreType.DMA((SLOTS,)),
        ],
        compiler_params=pltpu.CompilerParams(vmem_limit_bytes=44 * 1024 * 1024),
        name="attend",
    )(*(pltpu.with_memory_space_constraint(a, pltpu.HBM)
        for a in (lens, x, kc, vc, gain[None], bias[None], wq, bq[None], wkv, bkv[None])))


def merge_kernel(part, w_ref, x_ref, b_ref, out, near, mine, outbox, inbox, a_s, ys, yr, full, ss, rs):
    tp, sq = lax.axis_index("tp"), lax.axis_index("sq")
    mate = sq + 1 - 2 * lax.rem(sq, 2)
    across = lax.rem(sq + 2, 4)
    corner = 3 - sq
    units = part.shape[0] // 4
    rows = units * UNIT
    heads = part.shape[2]
    to_mate, to_across, to_twin = {"sq": mate}, {"sq": across}, {"tp": 1 - tp}
    lane = lax.broadcasted_iota(jnp.int32, (heads, LANES), 1)

    bar = pltpu.get_barrier_semaphore()
    for dev in (to_mate, to_across, to_twin):
        pl.semaphore_signal(bar, inc=1, device_id=dev, device_id_type=MESH)
    pl.semaphore_wait(bar, 3)

    def send(kind, k, src, dst, dev):
        return pltpu.make_async_remote_copy(src, dst, ss.at[kind, k], rs.at[kind, k], device_id=dev, device_id_type=MESH)

    def block(owner, k):
        return pl.ds(pl.multiple_of(owner * rows + k * UNIT, UNIT), UNIT)

    def c_near(k):
        return send(0, k, part.at[corner * units + k], near.at[k], to_mate)

    def c_mine(k):
        return send(1, k, part.at[mate * units + k], mine.at[k], to_mate)

    def c_cross(k):
        return send(2, k, outbox.at[k], inbox.at[k], to_across)

    def c_twin(k):
        r = pl.ds(k * UNIT, UNIT)
        return send(3, k, ys.at[r], yr.at[r], to_twin)

    def c_row(k):
        return send(4, k, full.at[block(sq, k)], full.at[block(sq, k)], to_across)

    def c_own(k):
        return send(5, k, full.at[block(sq, k)], full.at[block(sq, k)], to_mate)

    def c_pass(k):
        return send(6, k, full.at[block(across, k)], full.at[block(across, k)], to_mate)

    for k in range(units):
        c_near(k).start()
    for k in range(units):
        c_mine(k).start()

    def step_merge(k):
        c_near(k).wait_recv()
        own = across * units + k
        s0, s1 = part[own, UNIT], near[k, UNIT]
        top = jnp.maximum(s0, s1)
        e0, e1 = jnp.exp(s0 - top), jnp.exp(s1 - top)
        tot = pltpu.roll(s0, LANES - UNIT, 1) * e0 + pltpu.roll(s1, LANES - UNIT, 1) * e1
        for j in range(UNIT):
            outbox[k, j] = part[own, j] * e0[:, j:j + 1] + near[k, j] * e1[:, j:j + 1]
        outbox[k, UNIT] = jnp.where(lane < UNIT, top, jnp.where(lane < 2 * UNIT, pltpu.roll(tot, UNIT, 1), 0.0))
        c_cross(k).start()

    def step_combine(k):
        c_mine(k).wait_recv()
        c_cross(k).wait_recv()
        own = sq * units + k
        s0, s1, s2 = part[own, UNIT], mine[k, UNIT], inbox[k, UNIT]
        top = jnp.maximum(jnp.maximum(s0, s1), s2)
        e0, e1, e2 = jnp.exp(s0 - top), jnp.exp(s1 - top), jnp.exp(s2 - top)
        back = LANES - UNIT
        tot = pltpu.roll(s0, back, 1) * e0 + pltpu.roll(s1, back, 1) * e1 + pltpu.roll(s2, back, 1) * e2
        inv = 1.0 / jnp.where(lane < UNIT, tot, 1.0)
        e0, e1, e2 = e0 * inv, e1 * inv, e2 * inv
        for j in range(UNIT):
            a_s[k * UNIT + j] = part[own, j] * e0[:, j:j + 1] + mine[k, j] * e1[:, j:j + 1] + inbox[k, j] * e2[:, j:j + 1]

    def step_project(ks):
        r = pl.ds(ks[0] * UNIT, len(ks) * UNIT)
        lhs = jnp.concatenate([a_s[r, h, :].astype(BF16) for h in range(heads)], axis=1)
        ys[r, :] = jnp.dot(lhs, w_ref[...], preferred_element_type=F32)
        for k in ks:
            c_twin(k).start()

    def step_rows(k):
        c_twin(k).wait_recv()
        r = pl.ds(k * UNIT, UNIT)
        pair = x_ref[pl.ds(pl.multiple_of(sq * rows + (k // 2) * 2 * UNIT, 2 * UNIT), 2 * UNIT), :].astype(F32)
        half = pair[(k % 2) * UNIT:(k % 2 + 1) * UNIT]
        full[block(sq, k), :] = half + (ys[r, :] + yr[r, :]) + b_ref[...]
        c_row(k).start()
        c_own(k).start()

    def step_pass(k):
        c_row(k).wait_recv()
        c_pass(k).start()

    def step_store(owner, k2):
        r = pl.ds(pl.multiple_of(owner * rows + k2 * 2 * UNIT, 2 * UNIT), 2 * UNIT)
        out[r, :] = full[r, :].astype(BF16)

    for k in range(units):
        step_merge(k)
    for k in range(units):
        step_combine(k)
        step_project([k])
        if k >= 4:
            step_rows(k - 4)
        if k >= 6:
            step_pass(k - 6)
    for k in range(units - 4, units):
        step_rows(k)
        step_pass(k - 2)
    for k2 in range(units // 2):
        step_store(sq, k2)
    for k in range(units - 2, units):
        step_pass(k)
    for k2 in range(units // 2):
        step_store(across, k2)
    for k2 in range(units // 2):
        for k in (2 * k2, 2 * k2 + 1):
            c_own(k).wait_recv()
        step_store(mate, k2)
    for k2 in range(units // 2):
        for k in (2 * k2, 2 * k2 + 1):
            c_pass(k).wait_recv()
        step_store(corner, k2)
    for k in range(units):
        for c in (c_near, c_mine, c_cross, c_twin, c_row, c_own, c_pass):
            c(k).wait_send()


def merge(part, w_out, hidden, b_out):
    units = part.shape[0] // 4
    heads = part.shape[2]
    width = w_out.shape[1]
    rows = units * UNIT
    vmem = pl.BlockSpec(memory_space=pltpu.VMEM)
    box = pltpu.VMEM((units,) + part.shape[1:], F32)
    return pl.pallas_call(
        merge_kernel,
        out_shape=jax.ShapeDtypeStruct(hidden.shape, BF16),
        in_specs=[vmem] * 4,
        out_specs=vmem,
        scratch_shapes=[
            box, box, box, box, pltpu.VMEM((rows, heads, HEAD), F32), pltpu.VMEM((rows, width), F32), pltpu.VMEM((rows, width), F32),
            pltpu.VMEM((4 * rows, width), F32), pltpu.SemaphoreType.DMA((7, units)), pltpu.SemaphoreType.DMA((7, units)),
        ],
        compiler_params=pltpu.CompilerParams(collective_id=0, has_side_effects=True, vmem_limit_bytes=24 * 1024 * 1024),
        name="merge",
    )(part, w_out, hidden, b_out[None])


def solution(mesh):
    def local_step(hidden, cache_lens, k_cache, v_cache, ln_gain, ln_bias, w_query, b_query, w_kv, b_kv, w_out, b_out):
        key_new, val_new, part = attend(cache_lens, hidden, k_cache, v_cache, ln_gain, ln_bias, w_query, b_query, w_kv, b_kv)
        return merge(part, w_out, hidden, b_out), key_new, val_new

    cache_spec = P("dp", "sq", None)
    row_spec = P("dp", None)
    in_specs = (row_spec, P("dp"), cache_spec, cache_spec, P(None), P(None), P(None, "tp"), P("tp"), P(None, None), P(None), P("tp", None), P(None))
    out_specs = (row_spec, cache_spec, cache_spec)
    return jax.shard_map(local_step, mesh=mesh, in_specs=in_specs, out_specs=out_specs, check_vma=False)
```

```python
import functools
import jax
import jax.numpy as jnp
from jax import lax
from jax.experimental import pallas as pl
from jax.experimental.pallas import tpu as pltpu
from jax.sharding import PartitionSpec as P

MESH = pl.DeviceIdType.MESH
F32, BF16 = jnp.float32, jnp.bfloat16
CHUNK = 16
SLOTS = 14
LEAD = 9
UNIT = 8
GROUPS = CHUNK // UNIT
EARLY = 3
HEAD = 128
LANES = 128


def attend_kernel(seqs, lens_hbm, x_hbm, kc, vc, gain_hbm, bias_hbm, wq_hbm, bq_hbm, wkv_hbm, bkv_hbm, kn, vn, part, q_s, kv_s,
                  lens, gain, bias, bq, bkv, x_s, h_s, wq_s, wkv_s, kbuf, vbuf, sem_in, rk, rv, wk, wv):
    pos = kc.shape[1]
    heads = q_s.shape[1]
    chunks = 4 * EARLY
    me = lax.axis_index("sq")
    base = me * pos

    def place(i):
        return pl.multiple_of((i // EARLY) * (seqs // 4) + lax.rem(i, EARLY) * CHUNK, CHUNK)

    def read(i):
        s = lax.rem(i, SLOTS)
        rows = pl.ds(place(i), CHUNK)
        return (pltpu.make_async_copy(kc.at[rows], kbuf.at[s], rk.at[s]),
                pltpu.make_async_copy(vc.at[rows], vbuf.at[s], rv.at[s]))

    def write(i):
        s = lax.rem(i, SLOTS)
        rows = pl.ds(place(i), CHUNK)
        return (pltpu.make_async_copy(kbuf.at[s], kn.at[rows], wk.at[s]),
                pltpu.make_async_copy(vbuf.at[s], vn.at[rows], wv.at[s]))

    parts = wq_hbm.shape[1] // 256
    in_x = pltpu.make_async_copy(x_hbm, x_s, sem_in.at[0])
    in_kv = pltpu.make_async_copy(wkv_hbm, wkv_s, sem_in.at[1])
    in_q = [pltpu.make_async_copy(wq_hbm.at[:, pl.ds(g * 256, 256)], wq_s.at[:, pl.ds(g * 256, 256)], sem_in.at[2 + g])
            for g in range(parts)]
    small = [pltpu.make_async_copy(a, b, sem_in.at[8 + n])
             for n, (a, b) in enumerate(((gain_hbm, gain), (bias_hbm, bias), (bkv_hbm, bkv), (bq_hbm, bq), (lens_hbm, lens)))]
    in_x.start()
    for c in small:
        c.start()
    in_kv.start()
    for c in in_q:
        c.start()

    @pl.loop(0, min(LEAD, chunks))
    def _(i):
        for c in read(i):
            c.start()

    in_x.wait()
    for c in small:
        c.wait()
    rows_n = 32

    @pl.loop(0, x_s.shape[0] // rows_n)
    def _(r):
        rows = pl.ds(r * rows_n, rows_n)
        wide = x_s[rows, :].astype(F32)
        mean = jnp.mean(wide, axis=-1, keepdims=True)
        cent = wide - mean
        var = jnp.mean(cent * cent, axis=-1, keepdims=True)
        h_s[rows, :] = (cent * lax.rsqrt(var + 1e-5) * gain[...] + bias[...]).astype(BF16)

    in_kv.wait()
    kv_s[...] = (jnp.dot(h_s[...], wkv_s[...], preferred_element_type=F32) + bkv[...]).astype(BF16).astype(F32)
    for g in range(parts):
        in_q[g].wait()
        cols = slice(g * 256, (g + 1) * 256)
        q = (jnp.dot(h_s[...], wq_s[:, cols], preferred_element_type=F32) + bq[:, cols]).astype(BF16).astype(F32)
        q_s[:, 2 * g, :] = q[:, :HEAD]
        q_s[:, 2 * g + 1, :] = q[:, HEAD:]

    spot = lax.broadcasted_iota(jnp.int32, (heads, pos), 1) + base
    lane = lax.broadcasted_iota(jnp.int32, (heads, LANES), 1)
    row16 = lax.broadcasted_iota(jnp.int32, (16, HEAD), 0)
    def spread(i):
        return place(i), lax.rem(i, SLOTS)

    def values(i, weights):
        first, s = spread(i)
        for j in range(CHUNK):
            part[i * GROUPS + j // UNIT, j % UNIT] = jnp.dot(weights[j], vbuf[s, j], preferred_element_type=F32)

    def body(i, weights):
        first, s = spread(i)
        for c in read(i):
            c.wait()
        for j in range(CHUNK):
            b = first + j
            slot = lens[b] - base
            inside = jnp.logical_and(slot >= 0, slot < pos)
            at = pl.multiple_of(jnp.where(inside, slot // 16, 0) * 16, 16)
            mark = row16 == jnp.where(inside, slot - at, -1)
            win = pl.ds(at, 16)
            new = kv_s[pl.ds(b, 1), :].astype(BF16)
            kbuf[s, j, win, :] = jnp.where(mark, new[:, :HEAD], kbuf[s, j, win, :])
            vbuf[s, j, win, :] = jnp.where(mark, new[:, HEAD:], vbuf[s, j, win, :])
        scores = [lax.dot_general(q_s[first + j].astype(BF16), kbuf[s, j], (((1,), (1,)), ((), ())), preferred_element_type=F32)
                  for j in range(CHUNK)]
        values(jnp.maximum(i - 1, 0), weights)
        out = []
        for g in range(GROUPS):
            stat = jnp.zeros((heads, LANES), F32)
            for j in range(UNIT):
                valid = spot <= lens[first + g * UNIT + j]
                sc = jnp.where(valid, scores[g * UNIT + j] * (HEAD ** -0.5), -1e30)
                top = jnp.max(sc, axis=1, keepdims=True)
                w = jnp.where(valid, jnp.exp(sc - top), 0.0)
                tot = jnp.sum(w, axis=1, keepdims=True)
                out.append(w.astype(BF16))
                stat = jnp.where(lane == j, top, jnp.where(lane == UNIT + j, tot, stat))
            part[i * GROUPS + g, UNIT] = stat
        for c in write(i):
            c.start()
        ahead = i + LEAD

        @pl.when(ahead < chunks)
        def _():
            @pl.when(ahead >= SLOTS)
            def _():
                for c in write(ahead - SLOTS):
                    c.wait()
            for c in read(ahead):
                c.start()

        return tuple(out)

    last = lax.fori_loop(0, chunks, body, tuple(jnp.zeros((heads, pos), BF16) for _ in range(CHUNK)))
    values(chunks - 1, last)

    @pl.loop(max(0, chunks - SLOTS), chunks)
    def _(i):
        for c in write(i):
            c.wait()


def attend(lens, x, kc, vc, gain, bias, wq, bq, wkv, bkv):
    seqs, pos, _ = kc.shape
    heads = wq.shape[1] // HEAD
    width = x.shape[1]
    hbm = pl.BlockSpec(memory_space=pltpu.HBM)
    vmem = pl.BlockSpec(memory_space=pltpu.VMEM)
    return pl.pallas_call(
        functools.partial(attend_kernel, seqs),
        out_shape=(jax.ShapeDtypeStruct(kc.shape, BF16), jax.ShapeDtypeStruct(vc.shape, BF16),
                   jax.ShapeDtypeStruct((4 * EARLY * GROUPS, UNIT + 1, heads, HEAD), F32),
                   jax.ShapeDtypeStruct((seqs, heads, HEAD), F32), jax.ShapeDtypeStruct((seqs, 2 * HEAD), F32)),
        in_specs=[hbm] * 10,
        out_specs=(hbm, hbm, vmem, vmem, vmem),
        scratch_shapes=[
            pltpu.SMEM((seqs,), jnp.int32), pltpu.VMEM((1, width), F32), pltpu.VMEM((1, width), F32),
            pltpu.VMEM((1, wq.shape[1]), F32), pltpu.VMEM((1, 2 * HEAD), F32),
            pltpu.VMEM((seqs, width), BF16), pltpu.VMEM((seqs, width), BF16), pltpu.VMEM(wq.shape, BF16),
            pltpu.VMEM(wkv.shape, BF16),
            pltpu.VMEM((SLOTS, CHUNK, pos, HEAD), BF16), pltpu.VMEM((SLOTS, CHUNK, pos, HEAD), BF16),
            pltpu.SemaphoreType.DMA((13,)), pltpu.SemaphoreType.DMA((SLOTS,)), pltpu.SemaphoreType.DMA((SLOTS,)),
            pltpu.SemaphoreType.DMA((SLOTS,)), pltpu.SemaphoreType.DMA((SLOTS,)),
        ],
        compiler_params=pltpu.CompilerParams(vmem_limit_bytes=44 * 1024 * 1024),
        name="attend",
    )(*(pltpu.with_memory_space_constraint(a, pltpu.HBM)
        for a in (lens, x, kc, vc, gain[None], bias[None], wq, bq[None], wkv, bkv[None])))


PLAN = {
    3: [("merge", 0), ("merge", 1), ("merge", 2), ("merge", 3), ("merge", 4), ("merge", 5), ("attend", (6, 0)), ("attend", (6, 1)),
        ("project", [0]), ("attend", (7, 0)), ("project", [1, 2]), ("attend", (7, 1)), ("values", 0), ("merge", 6), ("project", [3, 4]),
        ("merge", 7), ("rows", 0), ("rows", 1), ("project", [5, 6]), ("rows", 2), ("rows", 3), ("project", [7]), ("pass", 0),
        ("rows", 4), ("pass", 1), ("rows", 5), ("pass", 2), ("rows", 6), ("pass", 3), ("rows", 7), ("pass", 4), ("store", 0),
        ("pass", 5), ("pass", 6), ("pass", 7), ("store", 1)],
    2: [("attend", (4, 0)), ("merge", 0), ("merge", 1), ("merge", 2), ("merge", 3), ("attend", (4, 1)), ("attend", (5, 0)), ("merge", 4),
        ("project", [0]), ("attend", (5, 1)), ("project", [1, 2]), ("attend", (6, 0)), ("merge", 5), ("rows", 0), ("attend", (6, 1)),
        ("project", [3, 4]), ("attend", (7, 0)), ("merge", 6), ("rows", 1), ("attend", (7, 1)), ("values", 0), ("rows", 2), ("project", [5]),
        ("merge", 7), ("rows", 3), ("project", [6]), ("pass", 0), ("rows", 4), ("pass", 1), ("project", [7]), ("pass", 2), ("rows", 5),
        ("pass", 3), ("rows", 6), ("pass", 4), ("rows", 7), ("store", 0), ("pass", 5), ("pass", 6), ("pass", 7), ("store", 1)],
}


def merge_kernel(part, q_ref, kv_ref, kc, vc, lens_hbm, w_ref, x_ref, b_ref, out, k2, v2,
                 lens, part2, near, mine, outbox, inbox, a_s, ys, yr, full, ss, rs, kr, vr, ls):
    tp, sq = lax.axis_index("tp"), lax.axis_index("sq")
    mate = sq + 1 - 2 * lax.rem(sq, 2)
    across = lax.rem(sq + 2, 4)
    corner = 3 - sq
    rows = x_ref.shape[0] // 4
    units = rows // UNIT
    early = part.shape[0] // 4
    late = units - early
    heads = part.shape[2]
    pos = kc.shape[1]
    base = sq * pos

    get_lens = pltpu.make_async_copy(lens_hbm, lens, ls.at[0])
    get_lens.start()

    def fetch(o, k):
        src, dst, n = pl.ds(o * rows + k * UNIT, UNIT), pl.ds((o * late + k - early) * UNIT, UNIT), o * late + k - early
        return (pltpu.make_async_copy(kc.at[src], k2.at[dst], kr.at[n]), pltpu.make_async_copy(vc.at[src], v2.at[dst], vr.at[n]))

    for k in range(early, units):
        for o in range(4):
            for c in fetch(o, k):
                c.start()

    def piece(o, k):
        return part.at[o * early + k] if k < early else part2.at[o * late + k - early]

    to_mate, to_across, to_twin = {"sq": mate}, {"sq": across}, {"tp": 1 - tp}
    lane = lax.broadcasted_iota(jnp.int32, (heads, LANES), 1)

    bar = pltpu.get_barrier_semaphore()
    for dev in (to_mate, to_across, to_twin):
        pl.semaphore_signal(bar, inc=1, device_id=dev, device_id_type=MESH)
    pl.semaphore_wait(bar, 3)

    def send(kind, k, src, dst, dev):
        return pltpu.make_async_remote_copy(src, dst, ss.at[kind, k], rs.at[kind, k], device_id=dev, device_id_type=MESH)

    def block(owner, k):
        return pl.ds(pl.multiple_of(owner * rows + k * UNIT, UNIT), UNIT)

    def c_near(k):
        return send(0, k, piece(corner, k), near.at[k], to_mate)

    def c_mine(k):
        return send(1, k, piece(mate, k), mine.at[k], to_mate)

    def c_cross(k):
        return send(2, k, outbox.at[k], inbox.at[k], to_across)

    def c_twin(k):
        r = pl.ds(k * UNIT, UNIT)
        return send(3, k, ys.at[r], yr.at[r], to_twin)

    def c_row(k):
        return send(4, k, full.at[block(sq, k)], full.at[block(sq, k)], to_across)

    def c_own(k):
        return send(5, k, full.at[block(sq, k)], full.at[block(sq, k)], to_mate)

    def c_pass(k):
        return send(6, k, full.at[block(across, k)], full.at[block(across, k)], to_mate)

    def step_near(k):
        c_near(k).start()
        c_mine(k).start()

    spot = lax.broadcasted_iota(jnp.int32, (heads, pos), 1)

    def step_values(k, pair, weights):
        for n, o in enumerate(pair):
            dst = piece(o, k)
            for j in range(UNIT):
                w, extra = weights[n * UNIT + j]
                dst[j] = jnp.dot(w, v2[(o * late + k - early) * UNIT + j], preferred_element_type=F32) + extra

    def step_attend(k, pair, before):
        for o in pair:
            for c in fetch(o, k):
                c.wait()
        where = [(o, o * rows + k * UNIT + j, (o * late + k - early) * UNIT + j) for o in pair for j in range(UNIT)]
        scores = [lax.dot_general(q_ref[b].astype(BF16), k2[n], (((1,), (1,)), ((), ())), preferred_element_type=F32)
                  for _, b, n in where]
        if before is not None:
            step_values(*before)
        weights = []
        stats = {o: jnp.zeros((heads, LANES), F32) for o in pair}
        for (o, b, _), sc in zip(where, scores):
            j = b % UNIT
            at = lens[b] - base
            new = kv_ref[b:b + 1, :]
            fresh = jnp.sum(q_ref[b] * new[:, :HEAD], axis=1, keepdims=True)
            here = spot == at
            sc = jnp.where(spot <= at, jnp.where(here, fresh, sc) * (HEAD ** -0.5), -1e30)
            top = jnp.max(sc, axis=1, keepdims=True)
            w = jnp.where(spot <= at, jnp.exp(sc - top), 0.0)
            tot = jnp.sum(w, axis=1, keepdims=True)
            mine_w = jnp.sum(jnp.where(here, w, 0.0), axis=1, keepdims=True)
            extra = mine_w.astype(BF16).astype(F32) * new[:, HEAD:]
            weights.append((jnp.where(here, 0.0, w).astype(BF16), extra))
            stats[o] = jnp.where(lane == j, top, jnp.where(lane == UNIT + j, tot, stats[o]))
        for o in pair:
            piece(o, k)[UNIT] = stats[o]
        return (k, pair, weights)

    def step_merge(k):
        c_near(k).wait_recv()
        own = piece(across, k)
        s0, s1 = own[UNIT], near[k, UNIT]
        top = jnp.maximum(s0, s1)
        e0, e1 = jnp.exp(s0 - top), jnp.exp(s1 - top)
        tot = pltpu.roll(s0, LANES - UNIT, 1) * e0 + pltpu.roll(s1, LANES - UNIT, 1) * e1
        for j in range(UNIT):
            outbox[k, j] = own[j] * e0[:, j:j + 1] + near[k, j] * e1[:, j:j + 1]
        outbox[k, UNIT] = jnp.where(lane < UNIT, top, jnp.where(lane < 2 * UNIT, pltpu.roll(tot, UNIT, 1), 0.0))
        c_cross(k).start()

    def step_combine(k):
        c_mine(k).wait_recv()
        c_cross(k).wait_recv()
        own = piece(sq, k)
        s0, s1, s2 = own[UNIT], mine[k, UNIT], inbox[k, UNIT]
        top = jnp.maximum(jnp.maximum(s0, s1), s2)
        e0, e1, e2 = jnp.exp(s0 - top), jnp.exp(s1 - top), jnp.exp(s2 - top)
        back = LANES - UNIT
        tot = pltpu.roll(s0, back, 1) * e0 + pltpu.roll(s1, back, 1) * e1 + pltpu.roll(s2, back, 1) * e2
        inv = 1.0 / jnp.where(lane < UNIT, tot, 1.0)
        e0, e1, e2 = e0 * inv, e1 * inv, e2 * inv
        for j in range(UNIT):
            a_s[k * UNIT + j] = own[j] * e0[:, j:j + 1] + mine[k, j] * e1[:, j:j + 1] + inbox[k, j] * e2[:, j:j + 1]

    def step_project(ks):
        r = pl.ds(ks[0] * UNIT, len(ks) * UNIT)
        lhs = jnp.concatenate([a_s[r, h, :].astype(BF16) for h in range(heads)], axis=1)
        ys[r, :] = jnp.dot(lhs, w_ref[...], preferred_element_type=F32)
        for k in ks:
            c_twin(k).start()

    def step_rows(k):
        c_twin(k).wait_recv()
        r = pl.ds(k * UNIT, UNIT)
        pair = x_ref[pl.ds(pl.multiple_of(sq * rows + (k // 2) * 2 * UNIT, 2 * UNIT), 2 * UNIT), :].astype(F32)
        half = pair[(k % 2) * UNIT:(k % 2 + 1) * UNIT]
        full[block(sq, k), :] = half + (ys[r, :] + yr[r, :]) + b_ref[...]
        c_row(k).start()
        c_own(k).start()

    def step_pass(k):
        c_row(k).wait_recv()
        c_pass(k).start()

    def step_store(owner, k2):
        r = pl.ds(pl.multiple_of(owner * rows + k2 * 2 * UNIT, 2 * UNIT), 2 * UNIT)
        out[r, :] = full[r, :].astype(BF16)

    for k in range(early):
        step_near(k)
    get_lens.wait()
    plan = PLAN[EARLY]
    before = None
    for name, k in plan:
        if name == "attend":
            k, half = k
            before = step_attend(k, ((0, 1), (2, 3))[half], before)
            if half == 0 and k > early:
                step_near(k - 1)
        elif name == "values":
            step_values(*before)
            step_near(units - 1)
        elif name == "merge":
            step_merge(k)
        elif name == "project":
            for n in k:
                step_combine(n)
            step_project(k)
        elif name == "rows":
            step_rows(k)
        elif name == "pass":
            step_pass(k)
        elif name == "store":
            for n in range(units // 2):
                step_store((sq, across)[k], n)
    for n in range(units // 2):
        for k in (2 * n, 2 * n + 1):
            c_own(k).wait_recv()
        step_store(mate, n)
    for n in range(units // 2):
        for k in (2 * n, 2 * n + 1):
            c_pass(k).wait_recv()
        step_store(corner, n)
    for k in range(units):
        for c in (c_near, c_mine, c_cross, c_twin, c_row, c_own, c_pass):
            c(k).wait_send()


def merge(part, q, kv, kc, vc, lens, w_out, hidden, b_out):
    heads = part.shape[2]
    seqs, width = hidden.shape
    rows = seqs // 4
    units = rows // UNIT
    left = seqs - 4 * EARLY * CHUNK
    vmem = pl.BlockSpec(memory_space=pltpu.VMEM)
    hbm = pl.BlockSpec(memory_space=pltpu.HBM)
    box = pltpu.VMEM((units,) + part.shape[1:], F32)
    pin = lambda a: pltpu.with_memory_space_constraint(a, pltpu.HBM)
    kept = pltpu.VMEM((left,) + kc.shape[1:], BF16)
    return pl.pallas_call(
        merge_kernel,
        out_shape=(jax.ShapeDtypeStruct(hidden.shape, BF16), kept, kept),
        in_specs=[vmem, vmem, vmem, hbm, hbm, hbm, vmem, vmem, vmem],
        out_specs=(vmem, vmem, vmem),
        scratch_shapes=[
            pltpu.SMEM((seqs,), jnp.int32), pltpu.VMEM((left // UNIT,) + part.shape[1:], F32),
            box, box, box, box, pltpu.VMEM((rows, heads, HEAD), F32), pltpu.VMEM((rows, width), F32), pltpu.VMEM((rows, width), F32),
            pltpu.VMEM((4 * rows, width), F32), pltpu.SemaphoreType.DMA((7, units)), pltpu.SemaphoreType.DMA((7, units)),
            pltpu.SemaphoreType.DMA((left // UNIT,)), pltpu.SemaphoreType.DMA((left // UNIT,)), pltpu.SemaphoreType.DMA((1,)),
        ],
        compiler_params=pltpu.CompilerParams(collective_id=0, has_side_effects=True, vmem_limit_bytes=16 * 1024 * 1024),
        name="merge",
    )(part, q, kv, pin(kc), pin(vc), pin(lens), w_out, hidden, b_out[None])


def store_kernel(kv, lens_hbm, y, k2_in, v2_in, kn_in, vn_in, kn, vn, y_out, k2, v2, lens, sem, wk, wv):
    del k2_in, v2_in, kn_in, vn_in
    seqs, pos = kn.shape[:2]
    own = seqs // 4
    left = k2.shape[0] // 4
    base = lax.axis_index("sq") * pos
    row16 = lax.broadcasted_iota(jnp.int32, (16, HEAD), 0)
    get_lens = pltpu.make_async_copy(lens_hbm, lens, sem.at[0])
    put_y = pltpu.make_async_copy(y, y_out, sem.at[1])
    get_lens.start()
    put_y.start()
    get_lens.wait()
    pieces = []
    for o in range(4):
        for n in range(left // CHUNK):
            first, kept = o * own + own - left + n * CHUNK, o * left + n * CHUNK
            for j in range(CHUNK):
                b = first + j
                slot = lens[b] - base
                inside = jnp.logical_and(slot >= 0, slot < pos)
                at = pl.multiple_of(jnp.where(inside, slot // 16, 0) * 16, 16)
                mark = row16 == jnp.where(inside, slot - at, -1)
                win = pl.ds(at, 16)
                new = kv[b:b + 1, :].astype(BF16)
                k2[kept + j, win, :] = jnp.where(mark, new[:, :HEAD], k2[kept + j, win, :])
                v2[kept + j, win, :] = jnp.where(mark, new[:, HEAD:], v2[kept + j, win, :])
            src, dst, m = pl.ds(kept, CHUNK), pl.ds(first, CHUNK), len(pieces) // 2
            pieces += [pltpu.make_async_copy(k2.at[src], kn.at[dst], wk.at[m]), pltpu.make_async_copy(v2.at[src], vn.at[dst], wv.at[m])]
            pieces[-2].start()
            pieces[-1].start()
    for c in pieces:
        c.wait()
    put_y.wait()


def store(kv, lens, y, k2, v2, kn, vn):
    vmem = pl.BlockSpec(memory_space=pltpu.VMEM)
    hbm = pl.BlockSpec(memory_space=pltpu.HBM)
    n = k2.shape[0] // CHUNK
    kept = pltpu.VMEM(k2.shape, BF16)
    return pl.pallas_call(
        store_kernel,
        out_shape=(jax.ShapeDtypeStruct(kn.shape, BF16), jax.ShapeDtypeStruct(vn.shape, BF16), jax.ShapeDtypeStruct(y.shape, BF16), kept, kept),
        in_specs=[vmem, hbm, vmem, vmem, vmem, hbm, hbm],
        out_specs=(hbm, hbm, hbm, vmem, vmem),
        input_output_aliases={3: 3, 4: 4, 5: 0, 6: 1},
        scratch_shapes=[pltpu.SMEM(lens.shape, jnp.int32), pltpu.SemaphoreType.DMA((2,)), pltpu.SemaphoreType.DMA((n,)), pltpu.SemaphoreType.DMA((n,))],
        compiler_params=pltpu.CompilerParams(vmem_limit_bytes=4 * 1024 * 1024),
        name="store",
    )(kv, pltpu.with_memory_space_constraint(lens, pltpu.HBM), y, k2, v2, kn, vn)[:3]


def solution(mesh):
    def local_step(hidden, cache_lens, k_cache, v_cache, ln_gain, ln_bias, w_query, b_query, w_kv, b_kv, w_out, b_out):
        key_part, val_part, part, q, kv = attend(cache_lens, hidden, k_cache, v_cache, ln_gain, ln_bias, w_query, b_query, w_kv, b_kv)
        y, k2, v2 = merge(part, q, kv, k_cache, v_cache, cache_lens, w_out, hidden, b_out)
        key_new, val_new, out = store(kv, cache_lens, y, k2, v2, key_part, val_part)
        return out, key_new, val_new

    cache_spec = P("dp", "sq", None)
    row_spec = P("dp", None)
    in_specs = (row_spec, P("dp"), cache_spec, cache_spec, P(None), P(None), P(None, "tp"), P("tp"), P(None, None), P(None), P("tp", None), P(None))
    out_specs = (row_spec, cache_spec, cache_spec)
    return jax.shard_map(local_step, mesh=mesh, in_specs=in_specs, out_specs=out_specs, check_vma=False)
```

```python
import functools
import jax
import jax.numpy as jnp
from jax import lax
from jax.experimental import pallas as pl
from jax.experimental.pallas import tpu as pltpu
from jax.sharding import PartitionSpec as P

MESH = pl.DeviceIdType.MESH
F32, BF16 = jnp.float32, jnp.bfloat16
CHUNK = 16
SLOTS = 14
LEAD = 9
UNIT = 8
GROUPS = CHUNK // UNIT
AHEAD = 3
EARLY = 2
HEAD = 128
LANES = 128
SHARED = 1
PLAN = [
    ("attend", (4, 0)), ("merge", 1), ("attend", (4, 1)), ("merge", 0), ("attend", (5, 0)), ("attend", (5, 1)), ("merge", 2),
    ("merge", 3), ("merge", 4), ("attend", (6, 0)), ("project", [0, 1]), ("attend", (6, 1)), ("attend", (7, 0)),
    ("merge", 5), ("attend", (7, 1)), ("merge", 6), ("values", 0), ("rows", 0), ("project", [2, 3]), ("rows", 1),
    ("merge", 7), ("merge", 8), ("project", [4]), ("project", [5, 6]), ("rows", 2), ("rows", 3), ("project", [7]),
    ("rows", 4), ("pass", 2), ("rows", 5), ("project", [8]), ("pass", 1), ("pass", 0), ("rows", 6), ("pass", 4), ("pass", 5),
    ("pass", 3), ("rows", 8), ("rows", 7), ("pass", 6),
]


def attend_kernel(seqs, lens_hbm, x_hbm, kc, vc, gain_hbm, bias_hbm, wq_hbm, bq_hbm, wkv_hbm, bkv_hbm, kn, vn, part, q_s, kv_s,
                  lens, gain, bias, bq, bkv, x_s, h_s, wq_s, wkv_s, kbuf, vbuf, sem_in, rk, rv, wk, wv):
    pos = kc.shape[1]
    heads = q_s.shape[1]
    chunks = 4 * EARLY
    me = lax.axis_index("sq")
    base = me * pos

    def place(i):
        return pl.multiple_of((i // EARLY) * (seqs // 4) + lax.rem(i, EARLY) * CHUNK, CHUNK)

    def read(i):
        s = lax.rem(i, SLOTS)
        rows = pl.ds(place(i), CHUNK)
        return (pltpu.make_async_copy(kc.at[rows], kbuf.at[s], rk.at[s]),
                pltpu.make_async_copy(vc.at[rows], vbuf.at[s], rv.at[s]))

    def write(i):
        s = lax.rem(i, SLOTS)
        rows = pl.ds(place(i), CHUNK)
        return (pltpu.make_async_copy(kbuf.at[s], kn.at[rows], wk.at[s]),
                pltpu.make_async_copy(vbuf.at[s], vn.at[rows], wv.at[s]))

    parts = wq_hbm.shape[1] // 256
    in_x = pltpu.make_async_copy(x_hbm, x_s, sem_in.at[0])
    in_kv = pltpu.make_async_copy(wkv_hbm, wkv_s, sem_in.at[1])
    in_q = [pltpu.make_async_copy(wq_hbm.at[:, pl.ds(g * 256, 256)], wq_s.at[:, pl.ds(g * 256, 256)], sem_in.at[2 + g])
            for g in range(parts)]
    small = [pltpu.make_async_copy(a, b, sem_in.at[8 + n])
             for n, (a, b) in enumerate(((gain_hbm, gain), (bias_hbm, bias), (bkv_hbm, bkv), (bq_hbm, bq), (lens_hbm, lens)))]
    in_x.start()
    for c in small:
        c.start()
    in_kv.start()
    for c in in_q:
        c.start()

    @pl.loop(0, min(LEAD, chunks))
    def _(i):
        for c in read(i):
            c.start()

    in_x.wait()
    for c in small:
        c.wait()
    rows_n = 32

    @pl.loop(0, x_s.shape[0] // rows_n)
    def _(r):
        rows = pl.ds(r * rows_n, rows_n)
        wide = x_s[rows, :].astype(F32)
        mean = jnp.mean(wide, axis=-1, keepdims=True)
        cent = wide - mean
        var = jnp.mean(cent * cent, axis=-1, keepdims=True)
        h_s[rows, :] = (cent * lax.rsqrt(var + 1e-5) * gain[...] + bias[...]).astype(BF16)

    in_kv.wait()
    kv_s[...] = (jnp.dot(h_s[...], wkv_s[...], preferred_element_type=F32) + bkv[...]).astype(BF16).astype(F32)
    for g in range(parts):
        in_q[g].wait()
        cols = slice(g * 256, (g + 1) * 256)
        q = (jnp.dot(h_s[...], wq_s[:, cols], preferred_element_type=F32) + bq[:, cols]).astype(BF16).astype(F32)
        q_s[:, 2 * g, :] = q[:, :HEAD]
        q_s[:, 2 * g + 1, :] = q[:, HEAD:]

    spot = lax.broadcasted_iota(jnp.int32, (heads, pos), 1) + base
    lane = lax.broadcasted_iota(jnp.int32, (heads, LANES), 1)
    row16 = lax.broadcasted_iota(jnp.int32, (16, HEAD), 0)
    def spread(i):
        return place(i), lax.rem(i, SLOTS)

    def values(i, weights):
        first, s = spread(i)
        for j in range(CHUNK):
            part[i * GROUPS + j // UNIT, j % UNIT] = jnp.dot(weights[j], vbuf[s, j], preferred_element_type=F32)

    def body(i, weights):
        first, s = spread(i)
        for c in read(i):
            c.wait()
        for j in range(CHUNK):
            b = first + j
            slot = lens[b] - base
            inside = jnp.logical_and(slot >= 0, slot < pos)
            at = pl.multiple_of(jnp.where(inside, slot // 16, 0) * 16, 16)
            mark = row16 == jnp.where(inside, slot - at, -1)
            win = pl.ds(at, 16)
            new = kv_s[pl.ds(b, 1), :].astype(BF16)
            kbuf[s, j, win, :] = jnp.where(mark, new[:, :HEAD], kbuf[s, j, win, :])
            vbuf[s, j, win, :] = jnp.where(mark, new[:, HEAD:], vbuf[s, j, win, :])
        scores = [lax.dot_general(q_s[first + j].astype(BF16), kbuf[s, j], (((1,), (1,)), ((), ())), preferred_element_type=F32)
                  for j in range(CHUNK)]
        values(jnp.maximum(i - 1, 0), weights)
        out = []
        for g in range(GROUPS):
            stat = jnp.zeros((heads, LANES), F32)
            for j in range(UNIT):
                valid = spot <= lens[first + g * UNIT + j]
                sc = jnp.where(valid, scores[g * UNIT + j] * (HEAD ** -0.5), -1e30)
                top = jnp.max(sc, axis=1, keepdims=True)
                w = jnp.where(valid, jnp.exp(sc - top), 0.0)
                tot = jnp.sum(w, axis=1, keepdims=True)
                out.append(w.astype(BF16))
                stat = jnp.where(lane == j, top, jnp.where(lane == UNIT + j, tot, stat))
            part[i * GROUPS + g, UNIT] = stat
        for c in write(i):
            c.start()
        ahead = i + LEAD

        @pl.when(ahead < chunks)
        def _():
            @pl.when(ahead >= SLOTS)
            def _():
                for c in write(ahead - SLOTS):
                    c.wait()
            for c in read(ahead):
                c.start()

        return tuple(out)

    last = lax.fori_loop(0, chunks, body, tuple(jnp.zeros((heads, pos), BF16) for _ in range(CHUNK)))
    values(chunks - 1, last)

    @pl.loop(max(0, chunks - SLOTS), chunks)
    def _(i):
        for c in write(i):
            c.wait()


def attend(lens, x, kc, vc, gain, bias, wq, bq, wkv, bkv):
    seqs, pos, _ = kc.shape
    heads = wq.shape[1] // HEAD
    width = x.shape[1]
    hbm = pl.BlockSpec(memory_space=pltpu.HBM)
    vmem = pl.BlockSpec(memory_space=pltpu.VMEM)
    return pl.pallas_call(
        functools.partial(attend_kernel, seqs),
        out_shape=(jax.ShapeDtypeStruct(kc.shape, BF16), jax.ShapeDtypeStruct(vc.shape, BF16),
                   jax.ShapeDtypeStruct((4 * EARLY * GROUPS, UNIT + 1, heads, HEAD), F32),
                   jax.ShapeDtypeStruct((seqs, heads, HEAD), F32), jax.ShapeDtypeStruct((seqs, 2 * HEAD), F32)),
        in_specs=[hbm] * 10,
        out_specs=(hbm, hbm, vmem, vmem, vmem),
        scratch_shapes=[
            pltpu.SMEM((seqs,), jnp.int32), pltpu.VMEM((1, width), F32), pltpu.VMEM((1, width), F32),
            pltpu.VMEM((1, wq.shape[1]), F32), pltpu.VMEM((1, 2 * HEAD), F32),
            pltpu.VMEM((seqs, width), BF16), pltpu.VMEM((seqs, width), BF16), pltpu.VMEM(wq.shape, BF16),
            pltpu.VMEM(wkv.shape, BF16),
            pltpu.VMEM((SLOTS, CHUNK, pos, HEAD), BF16), pltpu.VMEM((SLOTS, CHUNK, pos, HEAD), BF16),
            pltpu.SemaphoreType.DMA((13,)), pltpu.SemaphoreType.DMA((SLOTS,)), pltpu.SemaphoreType.DMA((SLOTS,)),
            pltpu.SemaphoreType.DMA((SLOTS,)), pltpu.SemaphoreType.DMA((SLOTS,)),
        ],
        compiler_params=pltpu.CompilerParams(vmem_limit_bytes=44 * 1024 * 1024),
        name="attend",
    )(*(pltpu.with_memory_space_constraint(a, pltpu.HBM)
        for a in (lens, x, kc, vc, gain[None], bias[None], wq, bq[None], wkv, bkv[None])))


def merge_kernel(part1, q_s, kv_s, kc, vc, lens_hbm, wo_s, x_s, bo, out, k2, v2,
                 lens, part2, near, mine, outbox, inbox, a_s, ys, yr, full, ss, rs, kr, vr, ls):
    tp, sq = lax.axis_index("tp"), lax.axis_index("sq")
    core = lax.rem(sq, 2)
    mate = sq + 1 - 2 * core
    across = lax.rem(sq + 2, 4)
    corner = 3 - sq
    rows = x_s.shape[0] // 4
    units = rows // UNIT
    early = part1.shape[0] // 4
    late = units - early
    alone = units - SHARED
    slots = alone + 2 * SHARED
    heads = q_s.shape[1]
    pos = kc.shape[1]
    base = sq * pos
    to_mate, to_across, to_twin = {"sq": mate}, {"sq": across}, {"tp": 1 - tp}
    lane = lax.broadcasted_iota(jnp.int32, (heads, LANES), 1)
    spot = lax.broadcasted_iota(jnp.int32, (heads, pos), 1)

    get_lens = pltpu.make_async_copy(lens_hbm, lens, ls.at[0])
    get_lens.start()

    def fetch(o, k):
        n = o * late + k - early
        src, dst = pl.ds(o * rows + k * UNIT, UNIT), pl.ds(n * UNIT, UNIT)
        return (pltpu.make_async_copy(kc.at[src], k2.at[dst], kr.at[n]), pltpu.make_async_copy(vc.at[src], v2.at[dst], vr.at[n]))

    halves = [(k, pair) for k in range(early, units) for pair in ((0, 1), (2, 3))]

    def begin(n):
        if n < len(halves):
            for o in halves[n][1]:
                for c in fetch(o, halves[n][0]):
                    c.start()

    for n in range(AHEAD):
        begin(n)

    bar = pltpu.get_barrier_semaphore()
    for dev in (to_mate, to_across, to_twin):
        pl.semaphore_signal(bar, inc=1, device_id=dev, device_id_type=MESH)
    pl.semaphore_wait(bar, 3)

    def send(kind, s, src, dst, dev):
        return pltpu.make_async_remote_copy(src, dst, ss.at[kind, s], rs.at[kind, s], device_id=dev, device_id_type=MESH)

    def unit_of(s):
        return s if s < alone else alone + (s - alone) % SHARED

    def owner_of(s, which):
        return which if s < alone else lax.rem(which, 2) + 2 * ((s - alone) // SHARED)

    def piece(o, k):
        return part1.at[o * early + k] if k < early else part2.at[o * late + k - early]

    def block(o, k):
        return pl.ds(pl.multiple_of(o * rows + k * UNIT, UNIT), UNIT)

    def c_near(s):
        return send(0, s, piece(owner_of(s, corner), unit_of(s)), near.at[s], to_mate)

    def c_mine(s):
        return send(1, s, piece(mate, s), mine.at[s], to_mate)

    def c_cross(s):
        return send(2, s, outbox.at[s], inbox.at[s], to_across)

    def c_twin(s):
        r = pl.ds(s * UNIT, UNIT)
        return send(3, s, ys.at[r], yr.at[r], to_twin)

    def c_row(s):
        return send(4, s, full.at[block(sq, s)], full.at[block(sq, s)], to_across)

    def c_own(s):
        r = block(owner_of(s, sq), unit_of(s))
        return send(5, s, full.at[r], full.at[r], to_mate)

    def c_pass(s):
        return send(6, s, full.at[block(across, s)], full.at[block(across, s)], to_mate)

    def step_near(k):
        for s in range(slots):
            if unit_of(s) == k:
                c_near(s).start()
                if s < alone:
                    c_mine(s).start()

    def step_values(k, pair, weights):
        for n, o in enumerate(pair):
            dst = piece(o, k)
            for j in range(UNIT):
                w, extra = weights[n * UNIT + j]
                dst[j] = jnp.dot(w, v2[(o * late + k - early) * UNIT + j], preferred_element_type=F32) + extra

    def step_attend(k, pair, before):
        begin(halves.index((k, pair)) + AHEAD)
        for o in pair:
            for c in fetch(o, k):
                c.wait()
        where = [(o, o * rows + k * UNIT + j, (o * late + k - early) * UNIT + j) for o in pair for j in range(UNIT)]
        scores = [lax.dot_general(q_s[b].astype(BF16), k2[n], (((1,), (1,)), ((), ())), preferred_element_type=F32) for _, b, n in where]
        if before is not None:
            step_values(*before)
        weights = []
        stats = {o: jnp.zeros((heads, LANES), F32) for o in pair}
        for (o, b, _), sc in zip(where, scores):
            j = b % UNIT
            at = lens[b] - base
            new = kv_s[b:b + 1, :]
            fresh = jnp.sum(q_s[b] * new[:, :HEAD], axis=1, keepdims=True)
            here = spot == at
            sc = jnp.where(spot <= at, jnp.where(here, fresh, sc) * (HEAD ** -0.5), -1e30)
            top = jnp.max(sc, axis=1, keepdims=True)
            w = jnp.where(spot <= at, jnp.exp(sc - top), 0.0)
            tot = jnp.sum(w, axis=1, keepdims=True)
            mine_w = jnp.sum(jnp.where(here, w, 0.0), axis=1, keepdims=True)
            extra = mine_w.astype(BF16).astype(F32) * new[:, HEAD:]
            weights.append((jnp.where(here, 0.0, w).astype(BF16), extra))
            stats[o] = jnp.where(lane == j, top, jnp.where(lane == UNIT + j, tot, stats[o]))
        for o in pair:
            piece(o, k)[UNIT] = stats[o]
        return (k, pair, weights)

    back = LANES - UNIT

    def step_merge(s):
        c_near(s).wait_recv()
        own = piece(owner_of(s, across), unit_of(s))
        s0, s1 = own[UNIT], near[s, UNIT]
        top = jnp.maximum(s0, s1)
        e0, e1 = jnp.exp(s0 - top), jnp.exp(s1 - top)
        tot = pltpu.roll(s0, back, 1) * e0 + pltpu.roll(s1, back, 1) * e1
        for j in range(UNIT):
            outbox[s, j] = own[j] * e0[:, j:j + 1] + near[s, j] * e1[:, j:j + 1]
        outbox[s, UNIT] = jnp.where(lane < UNIT, top, jnp.where(lane < 2 * UNIT, pltpu.roll(tot, UNIT, 1), 0.0))
        c_cross(s).start()

    def step_combine(s):
        c_cross(s).wait_recv()
        if s < alone:
            c_mine(s).wait_recv()
            boxes = [piece(sq, s), mine.at[s], inbox.at[s]]
        else:
            boxes = [outbox.at[s], inbox.at[s]]
        stats = [b[UNIT] for b in boxes]
        top = functools.reduce(jnp.maximum, stats)
        scales = [jnp.exp(t - top) for t in stats]
        tot = sum(pltpu.roll(t, back, 1) * e for t, e in zip(stats, scales))
        inv = 1.0 / jnp.where(lane < UNIT, tot, 1.0)
        scales = [e * inv for e in scales]
        for j in range(UNIT):
            a_s[s * UNIT + j] = sum(b[j] * e[:, j:j + 1] for b, e in zip(boxes, scales))

    def step_project(ss_):
        for s in ss_:
            step_combine(s)
        r = pl.ds(ss_[0] * UNIT, len(ss_) * UNIT)
        lhs = jnp.concatenate([a_s[r, h, :].astype(BF16) for h in range(heads)], axis=1)
        ys[r, :] = jnp.dot(lhs, wo_s[...], preferred_element_type=F32)
        for s in ss_:
            c_twin(s).start()

    def step_rows(s):
        c_twin(s).wait_recv()
        r = pl.ds(s * UNIT, UNIT)
        o, k = owner_of(s, sq), unit_of(s)
        pair = x_s[pl.ds(pl.multiple_of(o * rows + (k // 2) * 2 * UNIT, 2 * UNIT), 2 * UNIT), :].astype(F32)
        half = pair[(k % 2) * UNIT:(k % 2 + 1) * UNIT]
        full[block(o, k), :] = half + (ys[r, :] + yr[r, :]) + bo[...]
        if s < alone:
            c_row(s).start()
        c_own(s).start()

    def step_pass(s):
        c_row(s).wait_recv()
        c_pass(s).start()

    def step_store(o):
        for n in range(units // 2):
            r = pl.ds(pl.multiple_of(o * rows + n * 2 * UNIT, 2 * UNIT), 2 * UNIT)
            out[r, :] = full[r, :].astype(BF16)

    for k in range(early):
        step_near(k)
    get_lens.wait()
    before = None
    for name, k in PLAN:
        if name == "attend":
            k, half = k
            before = step_attend(k, ((0, 1), (2, 3))[half], before)
            if half == 0 and k > early:
                step_near(k - 1)
        elif name == "values":
            step_values(*before)
            step_near(units - 1)
        elif name == "merge":
            step_merge(k)
        elif name == "project":
            step_project(k)
        elif name == "rows":
            step_rows(k)
        elif name == "pass":
            step_pass(k)
    step_store(sq)
    step_store(across)
    for s in range(slots):
        c_own(s).wait_recv()
    step_store(mate)
    for s in range(alone):
        c_pass(s).wait_recv()
    step_store(corner)
    for s in range(slots):
        for c in (c_near, c_cross, c_twin, c_own) + ((c_mine, c_row, c_pass) if s < alone else ()):
            c(s).wait_send()


def merge(part, q, kv, kc, vc, lens, w_out, hidden, b_out):
    heads = part.shape[2]
    seqs, width = hidden.shape
    rows = seqs // 4
    units = rows // UNIT
    slots = units + SHARED
    left = seqs - 4 * EARLY * CHUNK
    vmem = pl.BlockSpec(memory_space=pltpu.VMEM)
    hbm = pl.BlockSpec(memory_space=pltpu.HBM)
    box = pltpu.VMEM((slots,) + part.shape[1:], F32)
    pin = lambda a: pltpu.with_memory_space_constraint(a, pltpu.HBM)
    kept = pltpu.VMEM((left,) + kc.shape[1:], BF16)
    return pl.pallas_call(
        merge_kernel,
        out_shape=(jax.ShapeDtypeStruct(hidden.shape, BF16), kept, kept),
        in_specs=[vmem, vmem, vmem, hbm, hbm, hbm, vmem, vmem, vmem],
        out_specs=(vmem, vmem, vmem),
        scratch_shapes=[
            pltpu.SMEM((seqs,), jnp.int32), pltpu.VMEM((left // UNIT,) + part.shape[1:], F32),
            box, box, box, box, pltpu.VMEM((slots * UNIT, heads, HEAD), F32), pltpu.VMEM((slots * UNIT, width), F32), pltpu.VMEM((slots * UNIT, width), F32),
            pltpu.VMEM((4 * rows, width), F32), pltpu.SemaphoreType.DMA((7, slots)), pltpu.SemaphoreType.DMA((7, slots)),
            pltpu.SemaphoreType.DMA((left // UNIT,)), pltpu.SemaphoreType.DMA((left // UNIT,)), pltpu.SemaphoreType.DMA((1,)),
        ],
        compiler_params=pltpu.CompilerParams(collective_id=0, has_side_effects=True, vmem_limit_bytes=16 * 1024 * 1024),
        name="merge",
    )(part, q, kv, pin(kc), pin(vc), pin(lens), w_out, hidden, b_out[None])


def store_kernel(kv, lens_hbm, y, k2_in, v2_in, kn_in, vn_in, kn, vn, y_out, k2, v2, lens, sem, wk, wv):
    del k2_in, v2_in, kn_in, vn_in
    seqs, pos = kn.shape[:2]
    own = seqs // 4
    left = k2.shape[0] // 4
    base = lax.axis_index("sq") * pos
    row16 = lax.broadcasted_iota(jnp.int32, (16, HEAD), 0)
    get_lens = pltpu.make_async_copy(lens_hbm, lens, sem.at[0])
    put_y = pltpu.make_async_copy(y, y_out, sem.at[1])
    get_lens.start()
    put_y.start()
    get_lens.wait()
    pieces = []
    for o in range(4):
        for n in range(left // CHUNK):
            first, kept = o * own + own - left + n * CHUNK, o * left + n * CHUNK
            for j in range(CHUNK):
                b = first + j
                slot = lens[b] - base
                inside = jnp.logical_and(slot >= 0, slot < pos)
                at = pl.multiple_of(jnp.where(inside, slot // 16, 0) * 16, 16)
                mark = row16 == jnp.where(inside, slot - at, -1)
                win = pl.ds(at, 16)
                new = kv[b:b + 1, :].astype(BF16)
                k2[kept + j, win, :] = jnp.where(mark, new[:, :HEAD], k2[kept + j, win, :])
                v2[kept + j, win, :] = jnp.where(mark, new[:, HEAD:], v2[kept + j, win, :])
            src, dst, m = pl.ds(kept, CHUNK), pl.ds(first, CHUNK), len(pieces) // 2
            pieces += [pltpu.make_async_copy(k2.at[src], kn.at[dst], wk.at[m]), pltpu.make_async_copy(v2.at[src], vn.at[dst], wv.at[m])]
            pieces[-2].start()
            pieces[-1].start()
    for c in pieces:
        c.wait()
    put_y.wait()


def store(kv, lens, y, k2, v2, kn, vn):
    vmem = pl.BlockSpec(memory_space=pltpu.VMEM)
    hbm = pl.BlockSpec(memory_space=pltpu.HBM)
    n = k2.shape[0] // CHUNK
    kept = pltpu.VMEM(k2.shape, BF16)
    return pl.pallas_call(
        store_kernel,
        out_shape=(jax.ShapeDtypeStruct(kn.shape, BF16), jax.ShapeDtypeStruct(vn.shape, BF16), jax.ShapeDtypeStruct(y.shape, BF16), kept, kept),
        in_specs=[vmem, hbm, vmem, vmem, vmem, hbm, hbm],
        out_specs=(hbm, hbm, hbm, vmem, vmem),
        input_output_aliases={3: 3, 4: 4, 5: 0, 6: 1},
        scratch_shapes=[pltpu.SMEM(lens.shape, jnp.int32), pltpu.SemaphoreType.DMA((2,)), pltpu.SemaphoreType.DMA((n,)), pltpu.SemaphoreType.DMA((n,))],
        compiler_params=pltpu.CompilerParams(vmem_limit_bytes=4 * 1024 * 1024),
        name="store",
    )(kv, pltpu.with_memory_space_constraint(lens, pltpu.HBM), y, k2, v2, kn, vn)[:3]


def solution(mesh):
    def local_step(hidden, cache_lens, k_cache, v_cache, ln_gain, ln_bias, w_query, b_query, w_kv, b_kv, w_out, b_out):
        key_part, val_part, part, q, kv = attend(cache_lens, hidden, k_cache, v_cache, ln_gain, ln_bias, w_query, b_query, w_kv, b_kv)
        y, k2, v2 = merge(part, q, kv, k_cache, v_cache, cache_lens, w_out, hidden, b_out)
        key_new, val_new, out = store(kv, cache_lens, y, k2, v2, key_part, val_part)
        return out, key_new, val_new

    cache_spec = P("dp", "sq", None)
    row_spec = P("dp", None)
    in_specs = (row_spec, P("dp"), cache_spec, cache_spec, P(None), P(None), P(None, "tp"), P("tp"), P(None, None), P(None), P("tp", None), P(None))
    out_specs = (row_spec, cache_spec, cache_spec)
    return jax.shard_map(local_step, mesh=mesh, in_specs=in_specs, out_specs=out_specs, check_vma=False)
```

```python
import functools
import jax
import jax.numpy as jnp
from jax import lax
from jax.experimental import pallas as pl
from jax.experimental.pallas import tpu as pltpu
from jax.sharding import PartitionSpec as P

MESH = pl.DeviceIdType.MESH
F32, BF16 = jnp.float32, jnp.bfloat16
CHUNK = 16
SLOTS = 14
LEAD = 12
UNIT = 8
GROUPS = CHUNK // UNIT
AHEAD = 3
EARLY = 2
HEAD = 128
LANES = 128
SOON = 2
SHARED = 2
PLAN = [
    ("attend", (4, 0)), ("attend", (4, 1)), ("merge", 1), ("merge", 0), ("merge", 2), ("attend", (5, 0)), ("attend", (5, 1)),
    ("attend", (6, 0)), ("merge", 3), ("attend", (6, 1)), ("project", [0, 1]), ("merge", 4), ("attend", (7, 0)),
    ("merge", 5), ("project", [2, 3]), ("merge", 8), ("merge", 6), ("attend", (7, 1)), ("values", 0), ("rows", 0),
    ("project", [4, 5]), ("merge", 9), ("rows", 1), ("merge", 7), ("project", [8]), ("rows", 2), ("project", [6]),
    ("rows", 4), ("project", [9]), ("rows", 3), ("rows", 5), ("pass", 1), ("project", [7]), ("pass", 3), ("rows", 9),
    ("rows", 6), ("rows", 8), ("pass", 2), ("pass", 4), ("pass", 0), ("pass", 5), ("rows", 7),
]


def attend_kernel(seqs, lens_hbm, x_hbm, kc, vc, gain_hbm, bias_hbm, wq_hbm, bq_hbm, wkv_hbm, bkv_hbm, kn, vn, part, q_s, kv_s,
                  lens, gain, bias, bq, bkv, x_s, h_s, wq_s, wkv_s, kbuf, vbuf, sem_in, rk, rv, wk, wv):
    pos = kc.shape[1]
    heads = q_s.shape[1]
    chunks = 4 * EARLY
    me = lax.axis_index("sq")
    base = me * pos

    def place(i):
        return pl.multiple_of((i // EARLY) * (seqs // 4) + lax.rem(i, EARLY) * CHUNK, CHUNK)

    def read(i):
        s = lax.rem(i, SLOTS)
        rows = pl.ds(place(i), CHUNK)
        return (pltpu.make_async_copy(kc.at[rows], kbuf.at[s], rk.at[s]),
                pltpu.make_async_copy(vc.at[rows], vbuf.at[s], rv.at[s]))

    def write(i):
        s = lax.rem(i, SLOTS)
        rows = pl.ds(place(i), CHUNK)
        return (pltpu.make_async_copy(kbuf.at[s], kn.at[rows], wk.at[s]),
                pltpu.make_async_copy(vbuf.at[s], vn.at[rows], wv.at[s]))

    parts = wq_hbm.shape[1] // 256
    in_x = pltpu.make_async_copy(x_hbm, x_s, sem_in.at[0])
    in_kv = pltpu.make_async_copy(wkv_hbm, wkv_s, sem_in.at[1])
    in_q = [pltpu.make_async_copy(wq_hbm.at[:, pl.ds(g * 256, 256)], wq_s.at[:, pl.ds(g * 256, 256)], sem_in.at[2 + g])
            for g in range(parts)]
    small = [pltpu.make_async_copy(a, b, sem_in.at[8 + n])
             for n, (a, b) in enumerate(((gain_hbm, gain), (bias_hbm, bias), (bkv_hbm, bkv), (bq_hbm, bq), (lens_hbm, lens)))]
    in_x.start()
    for c in small:
        c.start()
    in_kv.start()
    for c in in_q:
        c.start()

    @pl.loop(0, min(LEAD, chunks))
    def _(i):
        for c in read(i):
            c.start()

    in_x.wait()
    for c in small:
        c.wait()
    rows_n = 32

    @pl.loop(0, x_s.shape[0] // rows_n)
    def _(r):
        rows = pl.ds(r * rows_n, rows_n)
        wide = x_s[rows, :].astype(F32)
        mean = jnp.mean(wide, axis=-1, keepdims=True)
        cent = wide - mean
        var = jnp.mean(cent * cent, axis=-1, keepdims=True)
        h_s[rows, :] = (cent * lax.rsqrt(var + 1e-5) * gain[...] + bias[...]).astype(BF16)

    in_kv.wait()
    kv_s[...] = (jnp.dot(h_s[...], wkv_s[...], preferred_element_type=F32) + bkv[...]).astype(BF16).astype(F32)
    for g in range(parts):
        in_q[g].wait()
        cols = slice(g * 256, (g + 1) * 256)
        q = (jnp.dot(h_s[...], wq_s[:, cols], preferred_element_type=F32) + bq[:, cols]).astype(BF16).astype(F32)
        q_s[:, 2 * g, :] = q[:, :HEAD]
        q_s[:, 2 * g + 1, :] = q[:, HEAD:]

    spot = lax.broadcasted_iota(jnp.int32, (heads, pos), 1) + base
    lane = lax.broadcasted_iota(jnp.int32, (heads, LANES), 1)
    row16 = lax.broadcasted_iota(jnp.int32, (16, HEAD), 0)
    def spread(i):
        return place(i), lax.rem(i, SLOTS)

    def values(i, weights):
        first, s = spread(i)
        for j in range(CHUNK):
            part[i * GROUPS + j // UNIT, j % UNIT] = jnp.dot(weights[j], vbuf[s, j], preferred_element_type=F32)

    def body(i, weights):
        first, s = spread(i)
        for c in read(i):
            c.wait()
        for j in range(CHUNK):
            b = first + j
            slot = lens[b] - base
            inside = jnp.logical_and(slot >= 0, slot < pos)
            at = pl.multiple_of(jnp.where(inside, slot // 16, 0) * 16, 16)
            mark = row16 == jnp.where(inside, slot - at, -1)
            win = pl.ds(at, 16)
            new = kv_s[pl.ds(b, 1), :].astype(BF16)
            kbuf[s, j, win, :] = jnp.where(mark, new[:, :HEAD], kbuf[s, j, win, :])
            vbuf[s, j, win, :] = jnp.where(mark, new[:, HEAD:], vbuf[s, j, win, :])
        scores = [lax.dot_general(q_s[first + j].astype(BF16), kbuf[s, j], (((1,), (1,)), ((), ())), preferred_element_type=F32)
                  for j in range(CHUNK)]
        values(jnp.maximum(i - 1, 0), weights)
        out = []
        for g in range(GROUPS):
            stat = jnp.zeros((heads, LANES), F32)
            for j in range(UNIT):
                valid = spot <= lens[first + g * UNIT + j]
                sc = jnp.where(valid, scores[g * UNIT + j] * (HEAD ** -0.5), -1e30)
                top = jnp.max(sc, axis=1, keepdims=True)
                w = jnp.where(valid, jnp.exp(sc - top), 0.0)
                tot = jnp.sum(w, axis=1, keepdims=True)
                out.append(w.astype(BF16))
                stat = jnp.where(lane == j, top, jnp.where(lane == UNIT + j, tot, stat))
            part[i * GROUPS + g, UNIT] = stat
        for c in write(i):
            c.start()
        ahead = i + LEAD

        @pl.when(ahead < chunks)
        def _():
            @pl.when(ahead >= SLOTS)
            def _():
                for c in write(ahead - SLOTS):
                    c.wait()
            for c in read(ahead):
                c.start()

        return tuple(out)

    last = lax.fori_loop(0, chunks, body, tuple(jnp.zeros((heads, pos), BF16) for _ in range(CHUNK)))
    values(chunks - 1, last)

    @pl.loop(max(0, chunks - SLOTS), chunks)
    def _(i):
        for c in write(i):
            c.wait()


def attend(lens, x, kc, vc, gain, bias, wq, bq, wkv, bkv):
    seqs, pos, _ = kc.shape
    heads = wq.shape[1] // HEAD
    width = x.shape[1]
    hbm = pl.BlockSpec(memory_space=pltpu.HBM)
    vmem = pl.BlockSpec(memory_space=pltpu.VMEM)
    return pl.pallas_call(
        functools.partial(attend_kernel, seqs),
        out_shape=(jax.ShapeDtypeStruct(kc.shape, BF16), jax.ShapeDtypeStruct(vc.shape, BF16),
                   jax.ShapeDtypeStruct((4 * EARLY * GROUPS, UNIT + 1, heads, HEAD), F32),
                   jax.ShapeDtypeStruct((seqs, heads, HEAD), F32), jax.ShapeDtypeStruct((seqs, 2 * HEAD), F32)),
        in_specs=[hbm] * 10,
        out_specs=(hbm, hbm, vmem, vmem, vmem),
        scratch_shapes=[
            pltpu.SMEM((seqs,), jnp.int32), pltpu.VMEM((1, width), F32), pltpu.VMEM((1, width), F32),
            pltpu.VMEM((1, wq.shape[1]), F32), pltpu.VMEM((1, 2 * HEAD), F32),
            pltpu.VMEM((seqs, width), BF16), pltpu.VMEM((seqs, width), BF16), pltpu.VMEM(wq.shape, BF16),
            pltpu.VMEM(wkv.shape, BF16),
            pltpu.VMEM((SLOTS, CHUNK, pos, HEAD), BF16), pltpu.VMEM((SLOTS, CHUNK, pos, HEAD), BF16),
            pltpu.SemaphoreType.DMA((13,)), pltpu.SemaphoreType.DMA((SLOTS,)), pltpu.SemaphoreType.DMA((SLOTS,)),
            pltpu.SemaphoreType.DMA((SLOTS,)), pltpu.SemaphoreType.DMA((SLOTS,)),
        ],
        compiler_params=pltpu.CompilerParams(vmem_limit_bytes=44 * 1024 * 1024),
        name="attend",
    )(*(pltpu.with_memory_space_constraint(a, pltpu.HBM)
        for a in (lens, x, kc, vc, gain[None], bias[None], wq, bq[None], wkv, bkv[None])))


def merge_kernel(part1, q_s, kv_s, kc, vc, lens_hbm, wo_s, x_s, bo, out, k2, v2,
                 lens, part2, near, mine, outbox, inbox, a_s, ys, yr, full, ss, rs, kr, vr, ls):
    tp, sq = lax.axis_index("tp"), lax.axis_index("sq")
    core = lax.rem(sq, 2)
    mate = sq + 1 - 2 * core
    across = lax.rem(sq + 2, 4)
    corner = 3 - sq
    rows = x_s.shape[0] // 4
    units = rows // UNIT
    early = part1.shape[0] // 4
    late = units - early
    alone = units - SHARED
    slots = alone + 2 * SHARED
    heads = q_s.shape[1]
    pos = kc.shape[1]
    base = sq * pos
    to_mate, to_across, to_twin = {"sq": mate}, {"sq": across}, {"tp": 1 - tp}
    lane = lax.broadcasted_iota(jnp.int32, (heads, LANES), 1)
    spot = lax.broadcasted_iota(jnp.int32, (heads, pos), 1)

    get_lens = pltpu.make_async_copy(lens_hbm, lens, ls.at[0])
    get_lens.start()

    def fetch(o, k):
        n = o * late + k - early
        src, dst = pl.ds(o * rows + k * UNIT, UNIT), pl.ds(n * UNIT, UNIT)
        return (pltpu.make_async_copy(kc.at[src], k2.at[dst], kr.at[n]), pltpu.make_async_copy(vc.at[src], v2.at[dst], vr.at[n]))

    halves = [(k, pair) for k in range(early, units) for pair in ((0, 1), (2, 3))]

    def begin(n):
        if n < len(halves):
            for o in halves[n][1]:
                for c in fetch(o, halves[n][0]):
                    c.start()

    for n in range(AHEAD):
        begin(n)

    bar = pltpu.get_barrier_semaphore()
    for dev in (to_mate, to_across, to_twin):
        pl.semaphore_signal(bar, inc=1, device_id=dev, device_id_type=MESH)
    pl.semaphore_wait(bar, 3)

    def send(kind, s, src, dst, dev):
        return pltpu.make_async_remote_copy(src, dst, ss.at[kind, s], rs.at[kind, s], device_id=dev, device_id_type=MESH)

    def unit_of(s):
        return s if s < alone else alone + (s - alone) % SHARED

    def owner_of(s, which):
        return which if s < alone else lax.rem(which, 2) + 2 * ((s - alone) // SHARED)

    def piece(o, k):
        return part1.at[o * early + k] if k < early else part2.at[o * late + k - early]

    def block(o, k):
        return pl.ds(pl.multiple_of(o * rows + k * UNIT, UNIT), UNIT)

    def c_near(s):
        return send(0, s, piece(owner_of(s, corner), unit_of(s)), near.at[s], to_mate)

    def c_mine(s):
        return send(1, s, piece(mate, s), mine.at[s], to_mate)

    def c_cross(s):
        return send(2, s, outbox.at[s], inbox.at[s], to_across)

    def c_twin(s):
        r = pl.ds(s * UNIT, UNIT)
        return send(3, s, ys.at[r], yr.at[r], to_twin)

    def c_row(s):
        return send(4, s, full.at[block(sq, s)], full.at[block(sq, s)], to_across)

    def c_own(s):
        r = block(owner_of(s, sq), unit_of(s))
        return send(5, s, full.at[r], full.at[r], to_mate)

    def c_pass(s):
        return send(6, s, full.at[block(across, s)], full.at[block(across, s)], to_mate)

    def step_near(k):
        for s in range(slots):
            if unit_of(s) == k:
                c_near(s).start()
                if s < alone:
                    c_mine(s).start()

    def step_values(k, pair, weights):
        for n, o in enumerate(pair):
            dst = piece(o, k)
            for j in range(UNIT):
                w, extra = weights[n * UNIT + j]
                dst[j] = jnp.dot(w, v2[(o * late + k - early) * UNIT + j], preferred_element_type=F32) + extra

    def step_attend(k, pair, before):
        begin(halves.index((k, pair)) + AHEAD)
        for o in pair:
            for c in fetch(o, k):
                c.wait()
        where = [(o, o * rows + k * UNIT + j, (o * late + k - early) * UNIT + j) for o in pair for j in range(UNIT)]
        scores = [lax.dot_general(q_s[b].astype(BF16), k2[n], (((1,), (1,)), ((), ())), preferred_element_type=F32) for _, b, n in where]
        if before is not None:
            step_values(*before)
        weights = []
        stats = {o: jnp.zeros((heads, LANES), F32) for o in pair}
        for (o, b, _), sc in zip(where, scores):
            j = b % UNIT
            at = lens[b] - base
            new = kv_s[b:b + 1, :]
            fresh = jnp.sum(q_s[b] * new[:, :HEAD], axis=1, keepdims=True)
            here = spot == at
            sc = jnp.where(spot <= at, jnp.where(here, fresh, sc) * (HEAD ** -0.5), -1e30)
            top = jnp.max(sc, axis=1, keepdims=True)
            w = jnp.where(spot <= at, jnp.exp(sc - top), 0.0)
            tot = jnp.sum(w, axis=1, keepdims=True)
            mine_w = jnp.sum(jnp.where(here, w, 0.0), axis=1, keepdims=True)
            extra = mine_w.astype(BF16).astype(F32) * new[:, HEAD:]
            weights.append((jnp.where(here, 0.0, w).astype(BF16), extra))
            stats[o] = jnp.where(lane == j, top, jnp.where(lane == UNIT + j, tot, stats[o]))
        for o in pair:
            piece(o, k)[UNIT] = stats[o]
        return (k, pair, weights)

    back = LANES - UNIT

    def step_merge(s):
        c_near(s).wait_recv()
        own = piece(owner_of(s, across), unit_of(s))
        s0, s1 = own[UNIT], near[s, UNIT]
        top = jnp.maximum(s0, s1)
        e0, e1 = jnp.exp(s0 - top), jnp.exp(s1 - top)
        tot = pltpu.roll(s0, back, 1) * e0 + pltpu.roll(s1, back, 1) * e1
        for j in range(UNIT):
            outbox[s, j] = own[j] * e0[:, j:j + 1] + near[s, j] * e1[:, j:j + 1]
        outbox[s, UNIT] = jnp.where(lane < UNIT, top, jnp.where(lane < 2 * UNIT, pltpu.roll(tot, UNIT, 1), 0.0))
        c_cross(s).start()

    def step_combine(s):
        c_cross(s).wait_recv()
        if s < alone:
            c_mine(s).wait_recv()
            boxes = [piece(sq, s), mine.at[s], inbox.at[s]]
        else:
            boxes = [outbox.at[s], inbox.at[s]]
        stats = [b[UNIT] for b in boxes]
        top = functools.reduce(jnp.maximum, stats)
        scales = [jnp.exp(t - top) for t in stats]
        tot = sum(pltpu.roll(t, back, 1) * e for t, e in zip(stats, scales))
        inv = 1.0 / jnp.where(lane < UNIT, tot, 1.0)
        scales = [e * inv for e in scales]
        for j in range(UNIT):
            a_s[s * UNIT + j] = sum(b[j] * e[:, j:j + 1] for b, e in zip(boxes, scales))

    def step_project(ss_):
        for s in ss_:
            step_combine(s)
        r = pl.ds(ss_[0] * UNIT, len(ss_) * UNIT)
        lhs = jnp.concatenate([a_s[r, h, :].astype(BF16) for h in range(heads)], axis=1)
        ys[r, :] = jnp.dot(lhs, wo_s[...], preferred_element_type=F32)
        for s in ss_:
            c_twin(s).start()

    def step_rows(s):
        c_twin(s).wait_recv()
        r = pl.ds(s * UNIT, UNIT)
        o, k = owner_of(s, sq), unit_of(s)
        pair = x_s[pl.ds(pl.multiple_of(o * rows + (k // 2) * 2 * UNIT, 2 * UNIT), 2 * UNIT), :].astype(F32)
        half = pair[(k % 2) * UNIT:(k % 2 + 1) * UNIT]
        full[block(o, k), :] = half + (ys[r, :] + yr[r, :]) + bo[...]
        if s < alone:
            c_row(s).start()
        c_own(s).start()

    def step_pass(s):
        c_row(s).wait_recv()
        c_pass(s).start()

    def step_store(o):
        for n in range(units // 2):
            r = pl.ds(pl.multiple_of(o * rows + n * 2 * UNIT, 2 * UNIT), 2 * UNIT)
            out[r, :] = full[r, :].astype(BF16)

    for k in range(early):
        step_near(k)
    get_lens.wait()
    before = None
    for name, k in PLAN:
        if name == "attend":
            k, half = k
            before = step_attend(k, ((0, 1), (2, 3))[half], before)
            if half == 0 and k > early:
                step_near(k - 1)
        elif name == "values":
            step_values(*before)
            step_near(units - 1)
        elif name == "merge":
            step_merge(k)
        elif name == "project":
            step_project(k)
        elif name == "rows":
            step_rows(k)
        elif name == "pass":
            step_pass(k)
    step_store(sq)
    step_store(across)
    for s in range(slots):
        c_own(s).wait_recv()
    step_store(mate)
    for s in range(alone):
        c_pass(s).wait_recv()
    step_store(corner)
    for s in range(slots):
        for c in (c_near, c_cross, c_twin, c_own) + ((c_mine, c_row, c_pass) if s < alone else ()):
            c(s).wait_send()


def merge(part, q, kv, kc, vc, lens, w_out, hidden, b_out):
    heads = part.shape[2]
    seqs, width = hidden.shape
    rows = seqs // 4
    units = rows // UNIT
    slots = units + SHARED
    left = seqs - 4 * EARLY * CHUNK
    vmem = pl.BlockSpec(memory_space=pltpu.VMEM)
    hbm = pl.BlockSpec(memory_space=pltpu.HBM)
    box = pltpu.VMEM((slots,) + part.shape[1:], F32)
    pin = lambda a: pltpu.with_memory_space_constraint(a, pltpu.HBM)
    kept = pltpu.VMEM((left,) + kc.shape[1:], BF16)
    return pl.pallas_call(
        merge_kernel,
        out_shape=(jax.ShapeDtypeStruct(hidden.shape, BF16), kept, kept),
        in_specs=[vmem, vmem, vmem, hbm, hbm, hbm, vmem, vmem, vmem],
        out_specs=(vmem, vmem, vmem),
        scratch_shapes=[
            pltpu.SMEM((seqs,), jnp.int32), pltpu.VMEM((left // UNIT,) + part.shape[1:], F32),
            box, box, box, box, pltpu.VMEM((slots * UNIT, heads, HEAD), F32), pltpu.VMEM((slots * UNIT, width), F32), pltpu.VMEM((slots * UNIT, width), F32),
            pltpu.VMEM((4 * rows, width), F32), pltpu.SemaphoreType.DMA((7, slots)), pltpu.SemaphoreType.DMA((7, slots)),
            pltpu.SemaphoreType.DMA((left // UNIT,)), pltpu.SemaphoreType.DMA((left // UNIT,)), pltpu.SemaphoreType.DMA((1,)),
        ],
        compiler_params=pltpu.CompilerParams(collective_id=0, has_side_effects=True, vmem_limit_bytes=16 * 1024 * 1024),
        name="merge",
    )(part, q, kv, pin(kc), pin(vc), pin(lens), w_out, hidden, b_out[None])


def store_kernel(kv, lens_hbm, y, k2_in, v2_in, kn_in, vn_in, kn, vn, y_out, k2, v2, fix_k, fix_v, lens, sem, wk, wv, fk, fv):
    del k2_in, v2_in, kn_in, vn_in
    seqs, pos = kn.shape[:2]
    own = seqs // 4
    left = k2.shape[0] // 4
    base = lax.axis_index("sq") * pos
    row16 = lax.broadcasted_iota(jnp.int32, (16, HEAD), 0)
    get_lens = pltpu.make_async_copy(lens_hbm, lens, sem.at[0])
    put_y = pltpu.make_async_copy(y, y_out, sem.at[1])
    get_lens.start()
    put_y.start()
    places = [(o * own + own - left + n * CHUNK, o * left + n * CHUNK) for o in range(4) for n in range(left // CHUNK)]

    def put(m):
        first, kept = places[m]
        src, dst = pl.ds(kept, CHUNK), pl.ds(first, CHUNK)
        return pltpu.make_async_copy(k2.at[src], kn.at[dst], wk.at[m]), pltpu.make_async_copy(v2.at[src], vn.at[dst], wv.at[m])

    def window(b):
        slot = lens[b] - base
        inside = jnp.logical_and(slot >= 0, slot < pos)
        at = pl.multiple_of(jnp.where(inside, slot // 16, 0) * 16, 16)
        return row16 == jnp.where(inside, slot - at, -1), pl.ds(at, 16)

    def patch(m, j):
        b = places[m][0] + j
        _, win = window(b)
        return (pltpu.make_async_copy(fix_k.at[m * CHUNK + j], kn.at[b, win], fk.at[m]),
                pltpu.make_async_copy(fix_v.at[m * CHUNK + j], vn.at[b, win], fv.at[m]))

    for m in range(SOON):
        for c in put(m):
            c.start()
    get_lens.wait()
    for m in range(SOON, len(places)):
        first, kept = places[m]
        for j in range(CHUNK):
            mark, win = window(first + j)
            new = kv[first + j:first + j + 1, :].astype(BF16)
            k2[kept + j, win, :] = jnp.where(mark, new[:, :HEAD], k2[kept + j, win, :])
            v2[kept + j, win, :] = jnp.where(mark, new[:, HEAD:], v2[kept + j, win, :])
        for c in put(m):
            c.start()
    for m in range(SOON):
        first, kept = places[m]
        for j in range(CHUNK):
            mark, win = window(first + j)
            new = kv[first + j:first + j + 1, :].astype(BF16)
            fix_k[m * CHUNK + j] = jnp.where(mark, new[:, :HEAD], k2[kept + j, win, :])
            fix_v[m * CHUNK + j] = jnp.where(mark, new[:, HEAD:], v2[kept + j, win, :])
    for m in range(SOON):
        for c in put(m):
            c.wait()
        for j in range(CHUNK):
            for c in patch(m, j):
                c.start()
    for m in range(SOON, len(places)):
        for c in put(m):
            c.wait()
    for m in range(SOON):
        for j in range(CHUNK):
            for c in patch(m, j):
                c.wait()
    put_y.wait()


def store(kv, lens, y, k2, v2, kn, vn):
    vmem = pl.BlockSpec(memory_space=pltpu.VMEM)
    hbm = pl.BlockSpec(memory_space=pltpu.HBM)
    n = k2.shape[0] // CHUNK
    fix = pltpu.VMEM((SOON * CHUNK, 16, HEAD), BF16)
    kept = pltpu.VMEM(k2.shape, BF16)
    return pl.pallas_call(
        store_kernel,
        out_shape=(jax.ShapeDtypeStruct(kn.shape, BF16), jax.ShapeDtypeStruct(vn.shape, BF16), jax.ShapeDtypeStruct(y.shape, BF16), kept, kept),
        in_specs=[vmem, hbm, vmem, vmem, vmem, hbm, hbm],
        out_specs=(hbm, hbm, hbm, vmem, vmem),
        input_output_aliases={3: 3, 4: 4, 5: 0, 6: 1},
        scratch_shapes=[fix, fix, pltpu.SMEM(lens.shape, jnp.int32), pltpu.SemaphoreType.DMA((2,)), pltpu.SemaphoreType.DMA((n,)),
                        pltpu.SemaphoreType.DMA((n,)), pltpu.SemaphoreType.DMA((SOON,)), pltpu.SemaphoreType.DMA((SOON,))],
        compiler_params=pltpu.CompilerParams(vmem_limit_bytes=4 * 1024 * 1024),
        name="store",
    )(kv, pltpu.with_memory_space_constraint(lens, pltpu.HBM), y, k2, v2, kn, vn)[:3]


def solution(mesh):
    def local_step(hidden, cache_lens, k_cache, v_cache, ln_gain, ln_bias, w_query, b_query, w_kv, b_kv, w_out, b_out):
        key_part, val_part, part, q, kv = attend(cache_lens, hidden, k_cache, v_cache, ln_gain, ln_bias, w_query, b_query, w_kv, b_kv)
        y, k2, v2 = merge(part, q, kv, k_cache, v_cache, cache_lens, w_out, hidden, b_out)
        key_new, val_new, out = store(kv, cache_lens, y, k2, v2, key_part, val_part)
        return out, key_new, val_new

    cache_spec = P("dp", "sq", None)
    row_spec = P("dp", None)
    in_specs = (row_spec, P("dp"), cache_spec, cache_spec, P(None), P(None), P(None, "tp"), P("tp"), P(None, None), P(None), P("tp", None), P(None))
    out_specs = (row_spec, cache_spec, cache_spec)
    return jax.shard_map(local_step, mesh=mesh, in_specs=in_specs, out_specs=out_specs, check_vma=False)
```

```python
import functools
import jax
import jax.numpy as jnp
from jax import lax
from jax.experimental import pallas as pl
from jax.experimental.pallas import tpu as pltpu
from jax.sharding import PartitionSpec as P

MESH = pl.DeviceIdType.MESH
F32, BF16 = jnp.float32, jnp.bfloat16
CHUNK = 16
SLOTS = 14
LEAD = 12
UNIT = 8
GROUPS = CHUNK // UNIT
AHEAD = 2
EARLY = 2
HEAD = 128
LANES = 128
SOON = 2
SHARED = 2
PLAN = [
    ("attend", (4, 0)), ("attend", (4, 1)), ("merge", 1), ("merge", 0), ("merge", 2), ("attend", (5, 0)), ("attend", (5, 1)),
    ("attend", (6, 0)), ("merge", 3), ("attend", (6, 1)), ("project", [0, 1]), ("merge", 4), ("attend", (7, 0)),
    ("merge", 5), ("project", [2, 3]), ("merge", 8), ("merge", 6), ("attend", (7, 1)), ("values", 0), ("rows", 0),
    ("project", [4, 5]), ("merge", 9), ("rows", 1), ("merge", 7), ("project", [8]), ("rows", 2), ("project", [6]),
    ("rows", 4), ("project", [9]), ("rows", 3), ("rows", 5), ("pass", 1), ("project", [7]), ("pass", 3), ("rows", 9),
    ("rows", 6), ("rows", 8), ("pass", 2), ("pass", 4), ("pass", 0), ("pass", 5), ("rows", 7),
]


def attend_kernel(seqs, lens_hbm, x_hbm, kc, vc, gain_hbm, bias_hbm, wq_hbm, bq_hbm, wkv_hbm, bkv_hbm, kn, vn, part, q_s, kv_s,
                  lens, gain, bias, bq, bkv, x_s, h_s, wq_s, wkv_s, kbuf, vbuf, sem_in, rk, rv, wk, wv):
    pos = kc.shape[1]
    heads = q_s.shape[1]
    chunks = 4 * EARLY
    me = lax.axis_index("sq")
    base = me * pos

    def place(i):
        return pl.multiple_of((i // EARLY) * (seqs // 4) + lax.rem(i, EARLY) * CHUNK, CHUNK)

    def read(i):
        s = lax.rem(i, SLOTS)
        rows = pl.ds(place(i), CHUNK)
        return (pltpu.make_async_copy(kc.at[rows], kbuf.at[s], rk.at[s]),
                pltpu.make_async_copy(vc.at[rows], vbuf.at[s], rv.at[s]))

    def write(i):
        s = lax.rem(i, SLOTS)
        rows = pl.ds(place(i), CHUNK)
        return (pltpu.make_async_copy(kbuf.at[s], kn.at[rows], wk.at[s]),
                pltpu.make_async_copy(vbuf.at[s], vn.at[rows], wv.at[s]))

    parts = wq_hbm.shape[1] // 256
    in_x = pltpu.make_async_copy(x_hbm, x_s, sem_in.at[0])
    in_kv = pltpu.make_async_copy(wkv_hbm, wkv_s, sem_in.at[1])
    in_q = [pltpu.make_async_copy(wq_hbm.at[:, pl.ds(g * 256, 256)], wq_s.at[:, pl.ds(g * 256, 256)], sem_in.at[2 + g])
            for g in range(parts)]
    small = [pltpu.make_async_copy(a, b, sem_in.at[8 + n])
             for n, (a, b) in enumerate(((gain_hbm, gain), (bias_hbm, bias), (bkv_hbm, bkv), (bq_hbm, bq), (lens_hbm, lens)))]
    in_x.start()
    for c in small:
        c.start()
    in_kv.start()
    for c in in_q:
        c.start()

    @pl.loop(0, min(LEAD, chunks))
    def _(i):
        for c in read(i):
            c.start()

    in_x.wait()
    for c in small:
        c.wait()
    rows_n = 32

    @pl.loop(0, x_s.shape[0] // rows_n)
    def _(r):
        rows = pl.ds(r * rows_n, rows_n)
        wide = x_s[rows, :].astype(F32)
        mean = jnp.mean(wide, axis=-1, keepdims=True)
        cent = wide - mean
        var = jnp.mean(cent * cent, axis=-1, keepdims=True)
        h_s[rows, :] = (cent * lax.rsqrt(var + 1e-5) * gain[...] + bias[...]).astype(BF16)

    in_kv.wait()
    kv_s[...] = (jnp.dot(h_s[...], wkv_s[...], preferred_element_type=F32) + bkv[...]).astype(BF16).astype(F32)
    for g in range(parts):
        in_q[g].wait()
        cols = slice(g * 256, (g + 1) * 256)
        q = (jnp.dot(h_s[...], wq_s[:, cols], preferred_element_type=F32) + bq[:, cols]).astype(BF16).astype(F32)
        q_s[:, 2 * g, :] = q[:, :HEAD]
        q_s[:, 2 * g + 1, :] = q[:, HEAD:]

    spot = lax.broadcasted_iota(jnp.int32, (heads, pos), 1) + base
    lane = lax.broadcasted_iota(jnp.int32, (heads, LANES), 1)
    row16 = lax.broadcasted_iota(jnp.int32, (16, HEAD), 0)
    def spread(i):
        return place(i), lax.rem(i, SLOTS)

    def values(i, weights):
        first, s = spread(i)
        for j in range(CHUNK):
            part[i * GROUPS + j // UNIT, j % UNIT] = jnp.dot(weights[j], vbuf[s, j], preferred_element_type=F32)

    def body(i, weights):
        first, s = spread(i)
        for c in read(i):
            c.wait()
        for j in range(CHUNK):
            b = first + j
            slot = lens[b] - base
            inside = jnp.logical_and(slot >= 0, slot < pos)
            at = pl.multiple_of(jnp.where(inside, slot // 16, 0) * 16, 16)
            mark = row16 == jnp.where(inside, slot - at, -1)
            win = pl.ds(at, 16)
            new = kv_s[pl.ds(b, 1), :].astype(BF16)
            kbuf[s, j, win, :] = jnp.where(mark, new[:, :HEAD], kbuf[s, j, win, :])
            vbuf[s, j, win, :] = jnp.where(mark, new[:, HEAD:], vbuf[s, j, win, :])
        scores = [lax.dot_general(q_s[first + j].astype(BF16), kbuf[s, j], (((1,), (1,)), ((), ())), preferred_element_type=F32)
                  for j in range(CHUNK)]
        values(jnp.maximum(i - 1, 0), weights)
        out = []
        for g in range(GROUPS):
            stat = jnp.zeros((heads, LANES), F32)
            for j in range(UNIT):
                valid = spot <= lens[first + g * UNIT + j]
                sc = jnp.where(valid, scores[g * UNIT + j] * (HEAD ** -0.5), -1e30)
                top = jnp.max(sc, axis=1, keepdims=True)
                w = jnp.where(valid, jnp.exp(sc - top), 0.0)
                tot = jnp.sum(w, axis=1, keepdims=True)
                out.append(w.astype(BF16))
                stat = jnp.where(lane == j, top, jnp.where(lane == UNIT + j, tot, stat))
            part[i * GROUPS + g, UNIT] = stat
        for c in write(i):
            c.start()
        ahead = i + LEAD

        @pl.when(ahead < chunks)
        def _():
            @pl.when(ahead >= SLOTS)
            def _():
                for c in write(ahead - SLOTS):
                    c.wait()
            for c in read(ahead):
                c.start()

        return tuple(out)

    last = lax.fori_loop(0, chunks, body, tuple(jnp.zeros((heads, pos), BF16) for _ in range(CHUNK)))
    values(chunks - 1, last)

    @pl.loop(max(0, chunks - SLOTS), chunks)
    def _(i):
        for c in write(i):
            c.wait()


def attend(lens, x, kc, vc, gain, bias, wq, bq, wkv, bkv):
    seqs, pos, _ = kc.shape
    heads = wq.shape[1] // HEAD
    width = x.shape[1]
    hbm = pl.BlockSpec(memory_space=pltpu.HBM)
    vmem = pl.BlockSpec(memory_space=pltpu.VMEM)
    return pl.pallas_call(
        functools.partial(attend_kernel, seqs),
        out_shape=(jax.ShapeDtypeStruct(kc.shape, BF16), jax.ShapeDtypeStruct(vc.shape, BF16),
                   jax.ShapeDtypeStruct((4 * EARLY * GROUPS, UNIT + 1, heads, HEAD), F32),
                   jax.ShapeDtypeStruct((seqs, heads, HEAD), F32), jax.ShapeDtypeStruct((seqs, 2 * HEAD), F32)),
        in_specs=[hbm] * 10,
        out_specs=(hbm, hbm, vmem, vmem, vmem),
        scratch_shapes=[
            pltpu.SMEM((seqs,), jnp.int32), pltpu.VMEM((1, width), F32), pltpu.VMEM((1, width), F32),
            pltpu.VMEM((1, wq.shape[1]), F32), pltpu.VMEM((1, 2 * HEAD), F32),
            pltpu.VMEM((seqs, width), BF16), pltpu.VMEM((seqs, width), BF16), pltpu.VMEM(wq.shape, BF16),
            pltpu.VMEM(wkv.shape, BF16),
            pltpu.VMEM((SLOTS, CHUNK, pos, HEAD), BF16), pltpu.VMEM((SLOTS, CHUNK, pos, HEAD), BF16),
            pltpu.SemaphoreType.DMA((13,)), pltpu.SemaphoreType.DMA((SLOTS,)), pltpu.SemaphoreType.DMA((SLOTS,)),
            pltpu.SemaphoreType.DMA((SLOTS,)), pltpu.SemaphoreType.DMA((SLOTS,)),
        ],
        compiler_params=pltpu.CompilerParams(vmem_limit_bytes=44 * 1024 * 1024),
        name="attend",
    )(*(pltpu.with_memory_space_constraint(a, pltpu.HBM)
        for a in (lens, x, kc, vc, gain[None], bias[None], wq, bq[None], wkv, bkv[None])))


def merge_kernel(part1, q_s, kv_s, kc, vc, lens_hbm, wo_s, x_s, bo, out, k2, v2,
                 lens, part2, near, mine, outbox, inbox, a_s, ys, yr, full, ss, rs, kr, vr, ls):
    tp, sq = lax.axis_index("tp"), lax.axis_index("sq")
    core = lax.rem(sq, 2)
    mate = sq + 1 - 2 * core
    across = lax.rem(sq + 2, 4)
    corner = 3 - sq
    rows = x_s.shape[0] // 4
    units = rows // UNIT
    early = part1.shape[0] // 4
    late = units - early
    alone = units - SHARED
    slots = alone + 2 * SHARED
    heads = q_s.shape[1]
    pos = kc.shape[1]
    base = sq * pos
    to_mate, to_across, to_twin = {"sq": mate}, {"sq": across}, {"tp": 1 - tp}
    lane = lax.broadcasted_iota(jnp.int32, (heads, LANES), 1)
    spot = lax.broadcasted_iota(jnp.int32, (heads, pos), 1)

    get_lens = pltpu.make_async_copy(lens_hbm, lens, ls.at[0])
    get_lens.start()

    def fetch(o, k):
        n = o * late + k - early
        src, dst = pl.ds(o * rows + k * UNIT, UNIT), pl.ds(n * UNIT, UNIT)
        return (pltpu.make_async_copy(kc.at[src], k2.at[dst], kr.at[n]), pltpu.make_async_copy(vc.at[src], v2.at[dst], vr.at[n]))

    halves = [(k, pair) for k in range(early, units) for pair in ((0, 1), (2, 3))]

    def begin(n):
        if n < len(halves):
            for o in halves[n][1]:
                for c in fetch(o, halves[n][0]):
                    c.start()

    for n in range(AHEAD):
        begin(n)

    bar = pltpu.get_barrier_semaphore()
    for dev in (to_mate, to_across, to_twin):
        pl.semaphore_signal(bar, inc=1, device_id=dev, device_id_type=MESH)
    pl.semaphore_wait(bar, 3)

    def send(kind, s, src, dst, dev):
        return pltpu.make_async_remote_copy(src, dst, ss.at[kind, s], rs.at[kind, s], device_id=dev, device_id_type=MESH)

    def unit_of(s):
        return s if s < alone else alone + (s - alone) % SHARED

    def owner_of(s, which):
        return which if s < alone else lax.rem(which, 2) + 2 * ((s - alone) // SHARED)

    def piece(o, k):
        return part1.at[o * early + k] if k < early else part2.at[o * late + k - early]

    def block(o, k):
        return pl.ds(pl.multiple_of(o * rows + k * UNIT, UNIT), UNIT)

    def c_near(s):
        return send(0, s, piece(owner_of(s, corner), unit_of(s)), near.at[s], to_mate)

    def c_mine(s):
        return send(1, s, piece(mate, s), mine.at[s], to_mate)

    def c_cross(s):
        return send(2, s, outbox.at[s], inbox.at[s], to_across)

    def c_twin(s):
        r = pl.ds(s * UNIT, UNIT)
        return send(3, s, ys.at[r], yr.at[r], to_twin)

    def c_row(s):
        return send(4, s, full.at[block(sq, s)], full.at[block(sq, s)], to_across)

    def c_own(s):
        r = block(owner_of(s, sq), unit_of(s))
        return send(5, s, full.at[r], full.at[r], to_mate)

    def c_pass(s):
        return send(6, s, full.at[block(across, s)], full.at[block(across, s)], to_mate)

    def step_near(k):
        for s in range(slots):
            if unit_of(s) == k:
                c_near(s).start()
                if s < alone:
                    c_mine(s).start()

    def step_values(k, pair, weights):
        for n, o in enumerate(pair):
            dst = piece(o, k)
            for j in range(UNIT):
                w, extra = weights[n * UNIT + j]
                dst[j] = jnp.dot(w, v2[(o * late + k - early) * UNIT + j], preferred_element_type=F32) + extra

    def step_attend(k, pair, before):
        begin(halves.index((k, pair)) + AHEAD)
        for o in pair:
            for c in fetch(o, k):
                c.wait()
        where = [(o, o * rows + k * UNIT + j, (o * late + k - early) * UNIT + j) for o in pair for j in range(UNIT)]
        scores = [lax.dot_general(q_s[b].astype(BF16), k2[n], (((1,), (1,)), ((), ())), preferred_element_type=F32) for _, b, n in where]
        if before is not None:
            step_values(*before)
        weights = []
        stats = {o: jnp.zeros((heads, LANES), F32) for o in pair}
        for (o, b, _), sc in zip(where, scores):
            j = b % UNIT
            at = lens[b] - base
            new = kv_s[b:b + 1, :]
            fresh = jnp.sum(q_s[b] * new[:, :HEAD], axis=1, keepdims=True)
            here = spot == at
            sc = jnp.where(spot <= at, jnp.where(here, fresh, sc) * (HEAD ** -0.5), -1e30)
            top = jnp.max(sc, axis=1, keepdims=True)
            w = jnp.where(spot <= at, jnp.exp(sc - top), 0.0)
            tot = jnp.sum(w, axis=1, keepdims=True)
            mine_w = jnp.sum(jnp.where(here, w, 0.0), axis=1, keepdims=True)
            extra = mine_w.astype(BF16).astype(F32) * new[:, HEAD:]
            weights.append((jnp.where(here, 0.0, w).astype(BF16), extra))
            stats[o] = jnp.where(lane == j, top, jnp.where(lane == UNIT + j, tot, stats[o]))
        for o in pair:
            piece(o, k)[UNIT] = stats[o]
        return (k, pair, weights)

    back = LANES - UNIT

    def step_merge(s):
        c_near(s).wait_recv()
        own = piece(owner_of(s, across), unit_of(s))
        s0, s1 = own[UNIT], near[s, UNIT]
        top = jnp.maximum(s0, s1)
        e0, e1 = jnp.exp(s0 - top), jnp.exp(s1 - top)
        tot = pltpu.roll(s0, back, 1) * e0 + pltpu.roll(s1, back, 1) * e1
        for j in range(UNIT):
            outbox[s, j] = own[j] * e0[:, j:j + 1] + near[s, j] * e1[:, j:j + 1]
        outbox[s, UNIT] = jnp.where(lane < UNIT, top, jnp.where(lane < 2 * UNIT, pltpu.roll(tot, UNIT, 1), 0.0))
        c_cross(s).start()

    def step_combine(s):
        c_cross(s).wait_recv()
        if s < alone:
            c_mine(s).wait_recv()
            boxes = [piece(sq, s), mine.at[s], inbox.at[s]]
        else:
            boxes = [outbox.at[s], inbox.at[s]]
        stats = [b[UNIT] for b in boxes]
        top = functools.reduce(jnp.maximum, stats)
        scales = [jnp.exp(t - top) for t in stats]
        tot = sum(pltpu.roll(t, back, 1) * e for t, e in zip(stats, scales))
        inv = 1.0 / jnp.where(lane < UNIT, tot, 1.0)
        scales = [e * inv for e in scales]
        for j in range(UNIT):
            a_s[s * UNIT + j] = sum(b[j] * e[:, j:j + 1] for b, e in zip(boxes, scales))

    def step_project(ss_):
        for s in ss_:
            step_combine(s)
        r = pl.ds(ss_[0] * UNIT, len(ss_) * UNIT)
        lhs = jnp.concatenate([a_s[r, h, :].astype(BF16) for h in range(heads)], axis=1)
        ys[r, :] = jnp.dot(lhs, wo_s[...], preferred_element_type=F32)
        for s in ss_:
            c_twin(s).start()

    def step_rows(s):
        c_twin(s).wait_recv()
        r = pl.ds(s * UNIT, UNIT)
        o, k = owner_of(s, sq), unit_of(s)
        pair = x_s[pl.ds(pl.multiple_of(o * rows + (k // 2) * 2 * UNIT, 2 * UNIT), 2 * UNIT), :].astype(F32)
        half = pair[(k % 2) * UNIT:(k % 2 + 1) * UNIT]
        full[block(o, k), :] = half + (ys[r, :] + yr[r, :]) + bo[...]
        if s < alone:
            c_row(s).start()
        c_own(s).start()

    def step_pass(s):
        c_row(s).wait_recv()
        c_pass(s).start()

    def step_store(o):
        for n in range(units // 2):
            r = pl.ds(pl.multiple_of(o * rows + n * 2 * UNIT, 2 * UNIT), 2 * UNIT)
            out[r, :] = full[r, :].astype(BF16)

    for k in range(early):
        step_near(k)
    get_lens.wait()
    before = None
    for name, k in PLAN:
        if name == "attend":
            k, half = k
            before = step_attend(k, ((0, 1), (2, 3))[half], before)
            if half == 0 and k > early:
                step_near(k - 1)
        elif name == "values":
            step_values(*before)
            step_near(units - 1)
        elif name == "merge":
            step_merge(k)
        elif name == "project":
            step_project(k)
        elif name == "rows":
            step_rows(k)
        elif name == "pass":
            step_pass(k)
    step_store(sq)
    step_store(across)
    for s in range(slots):
        c_own(s).wait_recv()
    step_store(mate)
    for s in range(alone):
        c_pass(s).wait_recv()
    step_store(corner)
    for s in range(slots):
        for c in (c_near, c_cross, c_twin, c_own) + ((c_mine, c_row, c_pass) if s < alone else ()):
            c(s).wait_send()


def merge(part, q, kv, kc, vc, lens, w_out, hidden, b_out):
    heads = part.shape[2]
    seqs, width = hidden.shape
    rows = seqs // 4
    units = rows // UNIT
    slots = units + SHARED
    left = seqs - 4 * EARLY * CHUNK
    vmem = pl.BlockSpec(memory_space=pltpu.VMEM)
    hbm = pl.BlockSpec(memory_space=pltpu.HBM)
    box = pltpu.VMEM((slots,) + part.shape[1:], F32)
    pin = lambda a: pltpu.with_memory_space_constraint(a, pltpu.HBM)
    kept = pltpu.VMEM((left,) + kc.shape[1:], BF16)
    return pl.pallas_call(
        merge_kernel,
        out_shape=(jax.ShapeDtypeStruct(hidden.shape, BF16), kept, kept),
        in_specs=[vmem, vmem, vmem, hbm, hbm, hbm, vmem, vmem, vmem],
        out_specs=(vmem, vmem, vmem),
        scratch_shapes=[
            pltpu.SMEM((seqs,), jnp.int32), pltpu.VMEM((left // UNIT,) + part.shape[1:], F32),
            box, box, box, box, pltpu.VMEM((slots * UNIT, heads, HEAD), F32), pltpu.VMEM((slots * UNIT, width), F32), pltpu.VMEM((slots * UNIT, width), F32),
            pltpu.VMEM((4 * rows, width), F32), pltpu.SemaphoreType.DMA((7, slots)), pltpu.SemaphoreType.DMA((7, slots)),
            pltpu.SemaphoreType.DMA((left // UNIT,)), pltpu.SemaphoreType.DMA((left // UNIT,)), pltpu.SemaphoreType.DMA((1,)),
        ],
        compiler_params=pltpu.CompilerParams(collective_id=0, has_side_effects=True, vmem_limit_bytes=16 * 1024 * 1024),
        name="merge",
    )(part, q, kv, pin(kc), pin(vc), pin(lens), w_out, hidden, b_out[None])


def store_kernel(kv, lens_hbm, y, k2_in, v2_in, kn_in, vn_in, kn, vn, y_out, k2, v2, fix_k, fix_v, lens, sem, wk, wv, fk, fv):
    del k2_in, v2_in, kn_in, vn_in
    seqs, pos = kn.shape[:2]
    own = seqs // 4
    left = k2.shape[0] // 4
    base = lax.axis_index("sq") * pos
    row16 = lax.broadcasted_iota(jnp.int32, (16, HEAD), 0)
    get_lens = pltpu.make_async_copy(lens_hbm, lens, sem.at[0])
    put_y = pltpu.make_async_copy(y, y_out, sem.at[1])
    get_lens.start()
    put_y.start()
    places = [(o * own + own - left + n * CHUNK, o * left + n * CHUNK) for o in range(4) for n in range(left // CHUNK)]

    def put(m):
        first, kept = places[m]
        src, dst = pl.ds(kept, CHUNK), pl.ds(first, CHUNK)
        return pltpu.make_async_copy(k2.at[src], kn.at[dst], wk.at[m]), pltpu.make_async_copy(v2.at[src], vn.at[dst], wv.at[m])

    def window(b):
        slot = lens[b] - base
        inside = jnp.logical_and(slot >= 0, slot < pos)
        at = pl.multiple_of(jnp.where(inside, slot // 16, 0) * 16, 16)
        return row16 == jnp.where(inside, slot - at, -1), pl.ds(at, 16)

    def patch(m, j):
        b = places[m][0] + j
        _, win = window(b)
        return (pltpu.make_async_copy(fix_k.at[m * CHUNK + j], kn.at[b, win], fk.at[m]),
                pltpu.make_async_copy(fix_v.at[m * CHUNK + j], vn.at[b, win], fv.at[m]))

    for m in range(SOON):
        for c in put(m):
            c.start()
    get_lens.wait()
    for m in range(SOON, len(places)):
        first, kept = places[m]
        for j in range(CHUNK):
            mark, win = window(first + j)
            new = kv[first + j:first + j + 1, :].astype(BF16)
            k2[kept + j, win, :] = jnp.where(mark, new[:, :HEAD], k2[kept + j, win, :])
            v2[kept + j, win, :] = jnp.where(mark, new[:, HEAD:], v2[kept + j, win, :])
        for c in put(m):
            c.start()
    for m in range(SOON):
        first, kept = places[m]
        for j in range(CHUNK):
            mark, win = window(first + j)
            new = kv[first + j:first + j + 1, :].astype(BF16)
            fix_k[m * CHUNK + j] = jnp.where(mark, new[:, :HEAD], k2[kept + j, win, :])
            fix_v[m * CHUNK + j] = jnp.where(mark, new[:, HEAD:], v2[kept + j, win, :])
    for m in range(SOON):
        for c in put(m):
            c.wait()
        for j in range(CHUNK):
            for c in patch(m, j):
                c.start()
    for m in range(SOON, len(places)):
        for c in put(m):
            c.wait()
    for m in range(SOON):
        for j in range(CHUNK):
            for c in patch(m, j):
                c.wait()
    put_y.wait()


def store(kv, lens, y, k2, v2, kn, vn):
    vmem = pl.BlockSpec(memory_space=pltpu.VMEM)
    hbm = pl.BlockSpec(memory_space=pltpu.HBM)
    n = k2.shape[0] // CHUNK
    fix = pltpu.VMEM((SOON * CHUNK, 16, HEAD), BF16)
    kept = pltpu.VMEM(k2.shape, BF16)
    return pl.pallas_call(
        store_kernel,
        out_shape=(jax.ShapeDtypeStruct(kn.shape, BF16), jax.ShapeDtypeStruct(vn.shape, BF16), jax.ShapeDtypeStruct(y.shape, BF16), kept, kept),
        in_specs=[vmem, hbm, vmem, vmem, vmem, hbm, hbm],
        out_specs=(hbm, hbm, hbm, vmem, vmem),
        input_output_aliases={3: 3, 4: 4, 5: 0, 6: 1},
        scratch_shapes=[fix, fix, pltpu.SMEM(lens.shape, jnp.int32), pltpu.SemaphoreType.DMA((2,)), pltpu.SemaphoreType.DMA((n,)),
                        pltpu.SemaphoreType.DMA((n,)), pltpu.SemaphoreType.DMA((SOON,)), pltpu.SemaphoreType.DMA((SOON,))],
        compiler_params=pltpu.CompilerParams(vmem_limit_bytes=4 * 1024 * 1024),
        name="store",
    )(kv, pltpu.with_memory_space_constraint(lens, pltpu.HBM), y, k2, v2, kn, vn)[:3]


def solution(mesh):
    def local_step(hidden, cache_lens, k_cache, v_cache, ln_gain, ln_bias, w_query, b_query, w_kv, b_kv, w_out, b_out):
        key_part, val_part, part, q, kv = attend(cache_lens, hidden, k_cache, v_cache, ln_gain, ln_bias, w_query, b_query, w_kv, b_kv)
        y, k2, v2 = merge(part, q, kv, k_cache, v_cache, cache_lens, w_out, hidden, b_out)
        key_new, val_new, out = store(kv, cache_lens, y, k2, v2, key_part, val_part)
        return out, key_new, val_new

    cache_spec = P("dp", "sq", None)
    row_spec = P("dp", None)
    in_specs = (row_spec, P("dp"), cache_spec, cache_spec, P(None), P(None), P(None, "tp"), P("tp"), P(None, None), P(None), P("tp", None), P(None))
    out_specs = (row_spec, cache_spec, cache_spec)
    return jax.shard_map(local_step, mesh=mesh, in_specs=in_specs, out_specs=out_specs, check_vma=False)
```
